32 devices in a mesh: blk: 8 (over z, x), rep: 4 (over y, core).
Axes of the slice: x: 2, y: 2, z: 4, core: 2. Of those that a mesh axis runs over, the one named last changes fastest.
Arguments:
- embeddings: float32 [16384, 768], P(('blk', 'rep')), may hold values from -6 to 6
- ranks: int32 [16384], replicated, may hold values from 0 to 16383, each once
Outputs:
- earlier_best: float32 [16384], P(('blk', 'rep'))
- later_best: float32 [16384], P(('blk', 'rep'))
The draws below stay inside these ranges and needn't reach their ends.
Inputs may be any that keep to these rules, and one draw needn't show every extreme that they name: ranks is a permutation of 0 .. 16383.
All inputs are finite; a program needn't handle non-finite values.
Results may differ from the reference program's by a relative error of at most 0.0012.
Values may be sent and summed in bfloat16 or wider, within the bound.
A program may use at most 64 MiB of HBM per device.

```python
import jax
import jax.numpy as jnp
from jax import lax

D = 768
STEPS = 3
BLOCK = 2048
N = 16384
N_BLK = 8


def levels(rng, shape, cuts, low, top_value):
    def one(position, blocks):
        steps = jax.random.uniform(jax.random.fold_in(jax.random.fold_in(rng, 6), position), (blocks,), jnp.float32, low / len(cuts), top_value / len(cuts))
        return jnp.repeat(jnp.exp(steps), shape[position] // blocks).reshape((-1,) + (1,) * (len(shape) - position - 1))

    level = one(*cuts[0])
    for cut in cuts[1:]:
        level = level * one(*cut)
    return level


def noise(own_key, shape, spread, reach, shards=(), held_as=jnp.bfloat16):
    array = spread * jax.random.normal(own_key, shape, jnp.float32)
    if shards:
        array = array * levels(own_key, shape, shards, -0.22, 0.18)
    return jnp.clip(array, -reach, reach).astype(held_as)


def setup_inputs(seed: int = 0) -> dict:
    arg_keys = jax.random.split(jax.random.key(seed), 3)
    embeddings = noise(arg_keys[0], (N, D), 1.0, 6.0, ((0, 32),), jnp.float32)
    ranks = jax.random.permutation(arg_keys[1], N).astype(jnp.int32)
    return dict(embeddings=embeddings, ranks=ranks)


def reference(embeddings, ranks):
    squares = lax.optimization_barrier(jnp.sum(embeddings * embeddings, axis=1, keepdims=True))
    unit = (embeddings * lax.rsqrt(squares + 1e-06)).astype(jnp.bfloat16).astype(jnp.float32)
    units = unit.reshape(N_BLK, BLOCK, D)
    ordered = ranks.reshape(N_BLK, BLOCK)

    def one_block(index):
        host = units[index]
        host_rank = ordered[index]
        row_best = jnp.full((BLOCK,), -1.0, jnp.float32)
        columns = []
        for offset in range(STEPS + 1):
            other = (index - offset) % N_BLK
            scores = jnp.dot(host, units[other].T, precision=lax.Precision.HIGHEST, preferred_element_type=jnp.float32)
            kept = jnp.where(ordered[other][None, :] < host_rank[:, None], scores, jnp.float32(-1.0))
            row_best = jnp.maximum(row_best, lax.optimization_barrier(jnp.max(kept, axis=1)))
            columns.append(lax.optimization_barrier(jnp.max(kept, axis=0)))
        return (row_best, jnp.stack(columns))
    row_best, column_best = lax.map(one_block, jnp.arange(N_BLK, dtype=jnp.int32))
    later = column_best[:, 0]
    for offset in range(1, STEPS + 1):
        later = jnp.maximum(later, jnp.roll(column_best[:, offset], -offset, axis=0))
    return (row_best.reshape(N), later.reshape(N))
```

```python
import functools

import jax
import jax.numpy as jnp
from jax import lax
from jax.experimental import pallas as pl
from jax.experimental.pallas import tpu as pltpu
from jax.sharding import PartitionSpec as P

CHUNKS = 8
LANES = 128
MESH = pl.DeviceIdType.MESH


def kernel(
    blocks, copies, emb_hbm, ranks_hbm, early_ref, late_ref,
    emb, rank, host, vis, two,
    own_rank, vis_rank, two_rank,
    own_acc, vis_acc, two_acc, host_acc, swap_acc,
    row_out, row_in, back_out, back_in, two_out, two_in,
    emb_sem, rank_sem,
    core_send, core_recv, x_send, x_recv, y_send, y_recv, z_send, z_recv,
    relay_send, diag_send, diag_recv, twin_send, twin_recv, two_send, two_recv,
    row_send, row_sem, back_send, back_recv, twob_send, twob_recv,
):
    rows = emb.shape[0]
    part = rows // CHUNKS
    unit = rows // 2
    half = CHUNKS // 2
    lines = rows // LANES
    layers = blocks // 2
    wrap = layers == 4

    b = lax.axis_index("blk")
    r = lax.axis_index("rep")
    x = lax.rem(b, 2)
    l = b // 2
    other_x = 1 - x

    def flip_rep(k):
        dy, dc = k // 2, k % 2
        y, c = r // 2, lax.rem(r, 2)
        return 2 * (y + dy - 2 * y * dy) + c + dc - 2 * c * dc

    def flip_x(d):
        return x + d - 2 * x * d

    def peer(h):
        return (2 * l + flip_x(h // 4), flip_rep(h % 4))

    def layer(offset):
        return lax.rem(l + offset + layers, layers)

    if wrap:
        last = l // (layers - 1)
        is_relay = l == 1
        has_two = lax.rem(l, 2) == 0
    else:
        last = 0 * l
        is_relay = None
        has_two = None

    def if_relay(f):
        if wrap:
            pl.when(is_relay)(f)

    def if_two(f):
        if wrap:
            pl.when(has_two)(f)
        else:
            f()

    up = (2 * lax.rem(l + 1 + last, layers) + x, r)
    down = (2 * layer(-1) + x, r)
    far_up = (2 * layer(2) + x, r)
    far_down = (2 * layer(-2) + x, r)

    def cut(i):
        return pl.ds(pl.multiple_of(i * part, part), part)

    def emb_copy(i):
        return pltpu.make_async_copy(emb_hbm.at[cut(i)], emb.at[cut(i)], emb_sem.at[i])

    def rank_copy(k):
        size = 2 * copies * lines
        return pltpu.make_async_copy(
            ranks_hbm.at[pl.ds(pl.multiple_of(layer(-k) * size, size), size)], rank.at[k], rank_sem.at[k]
        )

    for i in range(CHUNKS):
        emb_copy(i).start()
    for k in range(3):
        rank_copy(k).start()

    barrier = pltpu.get_barrier_semaphore()
    greet = [peer(h) for h in range(1, 8)]
    for offset in (1, -1):
        greet.append((2 * layer(offset) + x, r))
    for offset in ((2,) if wrap else (2, -2)):
        greet.append((2 * layer(offset) + x, r))
        greet.append((2 * layer(offset) + other_x, r))
    for device in greet:
        pl.semaphore_signal(barrier, inc=1, device_id=device, device_id_type=MESH)

    def send(src, dst, send_sem, recv_sem, device):
        return pltpu.make_async_remote_copy(
            src_ref=src, dst_ref=dst, send_sem=send_sem, recv_sem=recv_sem,
            device_id=device, device_id_type=MESH,
        )

    def core_copy(i):
        return send(host.at[0, cut(i)], host.at[1, cut(i)], core_send.at[i], core_recv.at[i], peer(1))

    def x_copy(i):
        return send(host.at[0, cut(i)], host.at[4, cut(i)], x_send.at[i], x_recv.at[i], peer(4))

    def y_copy(i):
        return send(host.at[0, cut(i)], host.at[2, cut(i)], y_send.at[i], y_recv.at[i], peer(2))

    def z_copy(i):
        return send(host.at[0, cut(i)], vis.at[last, cut(i)], z_send.at[i], z_recv.at[last, i], up)

    def z_wait(slot, i):
        send(host.at[0, cut(i)], vis.at[slot, cut(i)], z_send.at[i], z_recv.at[slot, i], up).wait_recv()

    def relay_copy(i):
        return send(vis.at[1, cut(i)], vis.at[0, cut(i)], relay_send.at[i], z_recv.at[0, i], down)

    def diag_copy(i, by_x):
        src, device = (host.at[2, cut(i)], peer(4)) if by_x else (host.at[4, cut(i)], peer(2))
        return send(src, host.at[6, cut(i)], diag_send.at[i], diag_recv.at[i], device)

    def twin_copy(k, i):
        slot = 2 + 2 * k
        return send(host.at[slot, cut(i)], host.at[slot + 1, cut(i)], twin_send.at[k, i], twin_recv.at[k, i], peer(1))

    def two_copy(i):
        at = pl.ds(pl.multiple_of(x * unit + i * part, part), part)
        return send(host.at[4 * other_x, at], two.at[cut(i)], two_send.at[i], two_recv.at[i], far_up)

    def normalise(i):
        emb_copy(i).wait()
        v = emb[cut(i), :]
        squares = jnp.sum(v * v, axis=1, keepdims=True)
        host[0, cut(i), :] = (v * lax.rsqrt(squares + 1e-06)).astype(jnp.bfloat16)

    def launch(i):
        core_copy(i).start()
        x_copy(i).start()
        y_copy(i).start()
        z_copy(i).start()

    normalise(0)
    normalise(1)
    pl.semaphore_wait(barrier, len(greet))

    def prepare(i, _):
        launch(i - 2)
        normalise(i)
        return 0

    lax.fori_loop(2, CHUNKS, prepare, 0)

    for k in range(3):
        rank_copy(k).wait()
    launch(CHUNKS - 2)
    launch(CHUNKS - 1)

    sign = 2 * x - 1

    def spread(slot, row, count, out, factor=None):
        for g in range(count):
            line = rank[slot, pl.ds(row + g, 1), :]
            if factor is not None:
                line = line * factor
            out[g * LANES:(g + 1) * LANES, :] = jnp.broadcast_to(line, (LANES, LANES)).T

    mine = (copies * x + r) * lines
    spread(0, mine, lines, own_rank)
    own_acc[...] = jnp.full(own_acc.shape, -1.0, jnp.float32)
    vis_acc[...] = jnp.full(vis_acc.shape, -1.0, jnp.float32)
    two_acc[...] = jnp.full(two_acc.shape, -1.0, jnp.float32)
    host_acc[...] = jnp.full(host_acc.shape, -1.0, jnp.float32)
    swap_acc[...] = jnp.full(swap_acc.shape, -1.0, jnp.float32)

    def score(guest, guest_rank, guest_acc, h, u, acc, slot, factor=None):
        at = pl.ds(pl.multiple_of(u * unit, unit), unit)
        scores = lax.dot_general(
            guest[...], host[h, at, :], (((1,), (1,)), ((), ())), preferred_element_type=jnp.float32
        )
        row = (copies * flip_x(h // 4) + flip_rep(h % 4)) * lines + u * (unit // LANES)
        best = guest_acc[...]
        for g in range(unit // LANES):
            line = rank[0, pl.ds(row + g, 1), :]
            if factor is not None:
                line = line * factor
            kept = jnp.where(
                guest_rank[...] < line, scores[:, g * LANES:(g + 1) * LANES], jnp.float32(-1.0)
            )
            best = jnp.maximum(best, kept)
            column = jnp.max(kept.reshape(kept.shape[0] // 8, 8, LANES), axis=0)
            there = pl.ds(pl.multiple_of(u * unit + g * LANES, LANES), LANES)
            acc[slot, :, there] = jnp.maximum(acc[slot, :, there], column)
        guest_acc[...] = best

    def own_score(h, u):
        score(host.at[0], own_rank, own_acc, h, u, host_acc, h)

    def vis_score(h, u):
        score(vis.at[0], vis_rank.at[0], vis_acc.at[0], h, u, host_acc, h)

    def swap_score(h, u):
        score(vis.at[1], vis_rank.at[1], vis_acc.at[1], h, u, swap_acc, h - 4, sign)

    def two_score(h, u):
        score(two, two_rank, two_acc, h, u, host_acc, h)

    def sweep(f, low, high, first=0, count=2):
        def body(t, _):
            f(low + t // count, first + lax.rem(t, count))
            return 0
        lax.fori_loop(0, (high - low) * count, body, 0)

    sweep(own_score, 0, 1)
    spread(1, mine, lines, vis_rank.at[0])
    spread(2, mine, lines, vis_rank.at[1], sign)
    spread(2, (copies + r) * lines + x * (lines // 2), lines // 2, two_rank)

    def core_wait(i, _):
        core_copy(i).wait_recv()
        return 0

    lax.fori_loop(0, CHUNKS, core_wait, 0)
    sweep(own_score, 1, 2)

    def arrive(p, _):
        for by_x in (True, False):
            i = 2 * p + (0 if by_x else 1)
            y_copy(i).wait_recv()
            twin_copy(0, i).start()
            x_copy(i).wait_recv()
            twin_copy(1, i).start()
            diag_copy(i, by_x).start()

            @if_relay
            def _():
                z_wait(1, i)
                relay_copy(i).start()
        return 0

    def twins(k, first):
        def body(i, _):
            twin_copy(k, i).wait_recv()
            return 0
        lax.fori_loop(first, first + half, body, 0)

    for u in range(2):
        lax.fori_loop(u * (half // 2), (u + 1) * (half // 2), arrive, 0)
        if u == 1:
            @if_two
            def _():
                for i in range(half):
                    two_copy(i).start()
        twins(0, u * half)
        twins(1, u * half)
        sweep(own_score, 2, 4, u, 1)

        @pl.when(x == 0)
        def _():
            sweep(own_score, 4, 6, u, 1)

    def z_arrive(i, _):
        z_wait(0, i)
        return 0

    lax.fori_loop(0, CHUNKS, z_arrive, 0)
    sweep(vis_score, 0, 6)

    @if_relay
    def _():
        sweep(swap_score, 4, 6)

    def lanes(acc):
        return jnp.max(acc[...].T, axis=0, keepdims=True)

    def back_copy(slot):
        device = far_down if slot else (2 * lax.rem(l + layers - 1, layers) + x, r)
        return send(back_out.at[slot], back_in.at[slot], back_send.at[slot], back_recv.at[slot], device)

    def diag_arrive(i, _):
        diag_copy(i, True).wait_recv()
        twin_copy(2, i).start()
        return 0

    none = jnp.full((1, rows), -1.0, jnp.float32)
    for u in range(2):
        lax.fori_loop(u * half, (u + 1) * half, diag_arrive, 0)
        twins(2, u * half)
        sweep(vis_score, 6, 8, u, 1)
        if u == 1:
            back_out[0, 0:1, :] = none
            back_out[0, 1:2, :] = lanes(vis_acc.at[0])
            back_copy(0).start()

        @pl.when(x == 0)
        def _():
            sweep(own_score, 6, 8, u, 1)

        @if_relay
        def _():
            sweep(swap_score, 6, 8, u, 1)

    @if_relay
    def _():
        best = lanes(vis_acc.at[1])
        back_out[1, 0:1, :] = jnp.where(x == 0, best, none)
        back_out[1, 1:2, :] = jnp.where(x == 0, none, best)
        back_copy(1).start()

    @if_two
    def _():
        def two_arrive(i, _):
            two_copy(i).wait_recv()
            return 0
        lax.fori_loop(0, half, two_arrive, 0)

        def body(t, _):
            two_score(4 * x + t // 2, lax.rem(t, 2))
            return 0
        lax.fori_loop(0, 8, body, 0)

    def row_copy(h):
        return send(row_out.at[h - 1], row_in.at[h - 1], row_send.at[h - 1], row_sem.at[h - 1], peer(h))

    for h in range(7, 0, -1):
        best = jnp.max(host_acc[h], axis=0, keepdims=True)
        late = none
        if h >= 4 and wrap:
            swapped = jnp.max(swap_acc[h - 4], axis=0, keepdims=True)
            late = jnp.where(x == 0, swapped, none)
            best = jnp.where(x == 0, best, jnp.maximum(best, swapped))
        row_out[h - 1, 0:1, :] = best
        row_out[h - 1, 1:2, :] = late
        row_copy(h).start()

    def twob_copy(k):
        return send(two_out, two_in.at[k], twob_send, twob_recv.at[k], (2 * layer(-2) + 1, r))

    @if_two
    def _():
        two_out[...] = jnp.broadcast_to(lanes(two_acc), two_out.shape)
        twob_copy(x).start()

    early = jnp.max(host_acc[0], axis=0, keepdims=True)
    late = lanes(own_acc)
    early_ref[...] = early
    late_ref[...] = late

    def take(pair):
        early_ref[...] = jnp.maximum(early_ref[...], pair[0:1, :])
        late_ref[...] = jnp.maximum(late_ref[...], pair[1:2, :])

    for h in range(1, 8):
        row_copy(h).wait_recv()
        take(row_in.at[h - 1])
    back_copy(0).wait_recv()
    take(back_in.at[0])

    @if_two
    def _():
        @pl.when(x == 1)
        def _():
            for k in range(2):
                twob_copy(k).wait_recv()
                at = slice(k * unit, (k + 1) * unit)
                late_ref[:, at] = jnp.maximum(late_ref[:, at], two_in[k, 0:1, :])

    if wrap:
        @pl.when(l == layers - 1)
        def _():
            back_copy(1).wait_recv()
            take(back_in.at[1])

    def drain(i, _):
        core_copy(i).wait_send()
        x_copy(i).wait_send()
        y_copy(i).wait_send()
        z_copy(i).wait_send()
        diag_copy(i, True).wait_send()
        for k in range(3):
            twin_copy(k, i).wait_send()

        @if_relay
        def _():
            relay_copy(i).wait_send()
        return 0

    lax.fori_loop(0, CHUNKS, drain, 0)

    @if_two
    def _():
        for i in range(half):
            two_copy(i).wait_send()
        twob_copy(0).wait_send()

    for h in range(1, 8):
        row_copy(h).wait_send()
    back_copy(0).wait_send()

    @if_relay
    def _():
        back_copy(1).wait_send()


def shards(embeddings, ranks):
    rows, width = embeddings.shape
    copies = lax.axis_size("rep")
    blocks = lax.axis_size("blk")
    lines = rows // LANES
    dma = pltpu.SemaphoreType.DMA
    vmem = pl.BlockSpec(memory_space=pltpu.VMEM)
    hbm = pl.BlockSpec(memory_space=pltpu.HBM)
    f32, i32, bf16 = jnp.float32, jnp.int32, jnp.bfloat16
    half = CHUNKS // 2
    early, late = pl.pallas_call(
        functools.partial(kernel, blocks, copies),
        out_shape=[jax.ShapeDtypeStruct((1, rows), f32)] * 2,
        in_specs=[hbm, hbm],
        out_specs=[vmem, vmem],
        scratch_shapes=[
            pltpu.VMEM((rows, width), f32),
            pltpu.VMEM((3, 2 * copies * lines, LANES), i32),
            pltpu.VMEM((8, rows, width), bf16),
            pltpu.VMEM((2, rows, width), bf16),
            pltpu.VMEM((rows // 2, width), bf16),
            pltpu.VMEM((rows, LANES), i32),
            pltpu.VMEM((2, rows, LANES), i32),
            pltpu.VMEM((rows // 2, LANES), i32),
            pltpu.VMEM((rows, LANES), f32),
            pltpu.VMEM((2, rows, LANES), f32),
            pltpu.VMEM((rows // 2, LANES), f32),
            pltpu.VMEM((8, 8, rows), f32),
            pltpu.VMEM((4, 8, rows), f32),
            pltpu.VMEM((7, 2, rows), f32),
            pltpu.VMEM((7, 2, rows), f32),
            pltpu.VMEM((2, 2, rows), f32),
            pltpu.VMEM((2, 2, rows), f32),
            pltpu.VMEM((2, rows // 2), f32),
            pltpu.VMEM((2, 2, rows // 2), f32),
            dma((CHUNKS,)), dma((3,)),
            dma((CHUNKS,)), dma((CHUNKS,)), dma((CHUNKS,)), dma((CHUNKS,)),
            dma((CHUNKS,)), dma((CHUNKS,)), dma((CHUNKS,)), dma((2, CHUNKS)),
            dma((CHUNKS,)), dma((CHUNKS,)), dma((CHUNKS,)),
            dma((3, CHUNKS)), dma((3, CHUNKS)), dma((half,)), dma((half,)),
            dma((7,)), dma((7,)), dma((2,)), dma((2,)), dma, dma((2,)),
        ],
        compiler_params=pltpu.CompilerParams(
            collective_id=0, has_side_effects=True, vmem_limit_bytes=32 * 1024 * 1024
        ),
    )(embeddings, ranks.reshape(-1, LANES))
    return early.reshape(rows), late.reshape(rows)


def solution(mesh):
    return jax.shard_map(
        shards,
        mesh=mesh,
        in_specs=(P(("blk", "rep"), None), P()),
        out_specs=(P(("blk", "rep")), P(("blk", "rep"))),
        check_vma=False,
    )
```

```python
import functools

import jax
import jax.numpy as jnp
from jax import lax
from jax.experimental import pallas as pl
from jax.experimental.pallas import tpu as pltpu
from jax.sharding import PartitionSpec as P

CHUNKS = 8
LANES = 128
MESH = pl.DeviceIdType.MESH


def kernel(
    blocks, copies, emb_hbm, ranks_hbm, early_ref, late_ref,
    emb, rank, mem, pair, two,
    guest_rank, pair_rank, two_rank, guest_acc, pair_acc, two_acc, host_acc, swap_acc,
    row_out, row_in, back_out, back_in, two_out, two_in,
    emb_sem, rank_sem,
    core_send, core_recv, x_send, x_recv, y_send, y_recv, z_send, z_recv, pair_recv,
    relay_send, diag_send, diag_recv, twin_send, twin_recv, two_send, two_recv,
    row_send, row_sem, back_send, back_recv, twob_send, twob_recv,
):
    rows = emb.shape[0]
    part = rows // CHUNKS
    unit = rows // 2
    small = part // 2
    half = CHUNKS // 2
    lines = rows // LANES
    layers = blocks // 2
    wrap = layers == 4

    b = blocks - 1 - lax.axis_index("blk")
    r = lax.axis_index("rep")
    x = lax.rem(b, 2)
    l = b // 2

    def flip_rep(k):
        dy, dc = k // 2, k % 2
        y, c = r // 2, lax.rem(r, 2)
        return 2 * (y + dy - 2 * y * dy) + c + dc - 2 * c * dc

    def flip_x(d):
        return x + d - 2 * x * d

    def device(row, column, copy):
        return (blocks - 1 - 2 * row - column, copy)

    def peer(h):
        return device(l, flip_x(h // 4), flip_rep(h % 4))

    def layer(offset):
        return lax.rem(l + offset + layers, layers)

    if wrap:
        last = l // (layers - 1)
        is_relay = l == 1
        has_two = lax.rem(l, 2) == 0
    else:
        last = 0 * l
        is_relay = None
        has_two = None

    def if_relay(f):
        if wrap:
            pl.when(is_relay)(f)

    def unless_relay(f):
        if wrap:
            pl.when(l != 1)(f)
        else:
            f()

    def if_two(f):
        if wrap:
            pl.when(has_two)(f)
        else:
            f()

    up = device(layer(1), x, r)
    down = device(layer(-1), x, r)
    far_up = device(layer(2), x, r)
    far_down = device(layer(-2), x, r)

    def cut(i):
        return pl.ds(pl.multiple_of(i * part, part), part)

    def emb_copy(i):
        return pltpu.make_async_copy(emb_hbm.at[cut(i)], emb.at[cut(i)], emb_sem.at[i])

    def rank_copy(k):
        size = 2 * copies * lines
        return pltpu.make_async_copy(
            ranks_hbm.at[pl.ds(pl.multiple_of((layers - 1 - layer(-k)) * size, size), size)],
            rank.at[k], rank_sem,
        )

    barrier = pltpu.get_barrier_semaphore()

    def greet(target):
        pl.semaphore_signal(barrier, inc=1, device_id=target, device_id_type=MESH)

    for h in (1, 2, 4):
        greet(peer(h))
    if wrap:
        @pl.when(l == 0)
        def _():
            greet(device(l + 1, x, r))

        @pl.when(l > 0)
        def _():
            greet(down)

        @pl.when(l < layers - 1)
        def _():
            greet(far_up)
        expected = 5 - last
    else:
        greet(down)
        greet(far_down)
        expected = 5

    for i in range(CHUNKS):
        emb_copy(i).start()
    for k in range(3):
        rank_copy(k).start()

    def send(src, dst, send_sem, recv_sem, device):
        return pltpu.make_async_remote_copy(
            src_ref=src, dst_ref=dst, send_sem=send_sem, recv_sem=recv_sem,
            device_id=device, device_id_type=MESH,
        )

    def host(h):
        return mem.at[h + 1]

    def area(u):
        return pl.ds(u * unit, unit)

    every = pl.ds(0, rows)

    def core_copy(at):
        return send(host(0).at[at], host(1).at[at], core_send, core_recv, peer(1))

    def x_copy(i, at=None):
        at = cut(i) if at is None else at
        return send(host(0).at[at], host(4).at[at], x_send, x_recv.at[i], peer(4))

    def y_copy(i, at=None):
        at = cut(i) if at is None else at
        return send(host(0).at[at], host(2).at[at], y_send, y_recv.at[i], peer(2))

    def z_copy(u, at):
        return send(host(0).at[at], mem.at[0, at], z_send, z_recv.at[u], up)

    def far_copy(k, at):
        return send(host(0).at[at], pair.at[at], z_send, pair_recv.at[k], far_down)

    def relay_copy(u, at):
        return send(pair.at[at], mem.at[0, at], relay_send, z_recv.at[u], down)

    def diag_copy(i, by_x, at=None):
        at = cut(i) if at is None else at
        source, target = (2, peer(4)) if by_x else (4, peer(2))
        return send(host(source).at[at], host(6).at[at], diag_send, diag_recv.at[i], target)

    def twin_copy(k, u, at):
        slot = 2 + 2 * k
        return send(
            host(slot).at[at], host(slot + 1).at[at], twin_send.at[k], twin_recv.at[k, u], peer(1)
        )

    def two_copy(i, size):
        at = pl.ds(pl.multiple_of(x * unit + i * part, part), size)
        there = pl.ds(i * part, size)
        return send(host(4 * (1 - x)).at[at], two.at[there], two_send, two_recv, far_up)

    def normalise(i):
        emb_copy(i).wait()
        v = emb[cut(i), :]
        squares = jnp.sum(v * v, axis=1, keepdims=True)
        mem[1, cut(i), :] = (v * lax.rsqrt(squares + 1e-06)).astype(jnp.bfloat16)

    def piece(k):
        return pl.ds(pl.multiple_of(k * small, small), small)

    def ascend(i):
        def far():
            for n in range(part // small):
                k = i * (part // small) + n
                far_copy(k, piece(k)).start()

        if wrap:
            pl.when(last == 1)(far)

            @pl.when(last == 0)
            def _():
                z_copy(i // half, cut(i)).start()
        else:
            z_copy(i // half, cut(i)).start()

    def launch(i):
        ascend(i)
        x_copy(i).start()
        y_copy(i).start()
        core_copy(cut(i)).start()

    with jax.named_scope("norm"):
        normalise(0)
        normalise(1)
    with jax.named_scope("barrier"):
        pl.semaphore_wait(barrier, expected)

    def prepare(i, _):
        launch(i - 2)
        normalise(i)
        return 0

    with jax.named_scope("prepare"):
        launch(0)
        normalise(2)
        lax.fori_loop(3, CHUNKS, prepare, 0)
        for k in range(3):
            rank_copy(k).wait()
        launch(CHUNKS - 2)
        launch(CHUNKS - 1)

    def relay(i):
        for n in range(part // small):
            k = i * (part // small) + n
            with jax.named_scope("w"):
                far_copy(k, piece(k)).wait_recv()
            relay_copy(i // half, piece(k)).start()

    sign = 2 * x - 1

    def place(column, copy):
        return (copies * (1 - column) + copy) * lines

    def spread(slot, row, count, out, factor=None):
        for g in range(count):
            line = rank[slot, pl.ds(row + g, 1), :]
            if factor is not None:
                line = line * factor
            out[g * LANES:(g + 1) * LANES, :] = jnp.broadcast_to(line, (LANES, LANES)).T

    spread(0, place(x, r), lines, guest_rank.at[1])
    for acc in (guest_acc, pair_acc, two_acc, host_acc, swap_acc):
        acc[...] = jnp.full(acc.shape, -1.0, jnp.float32)

    def score(guest, guest_line, best_ref, h, u, acc, slot, factor=None, slots=1):
        if u is None:
            low, size = 0, rows
            hosts = mem[pl.ds(h + 1, slots)].reshape(slots * rows, mem.shape[2])
        else:
            low, size = u * unit, unit
            hosts = mem[h + 1, area(u), :]
        count = guest_line.size // LANES
        lhs = guest[...].reshape(count, hosts.shape[1])
        scores = lax.dot_general(
            lhs, hosts, (((1,), (1,)), ((), ())), preferred_element_type=jnp.float32
        )
        own = guest_line[...].reshape(count, LANES)
        best = best_ref[...].reshape(count, LANES)
        for k in range(slots):
            row = place(flip_x((h + k) // 4), flip_rep((h + k) % 4))
            for g in range(size // LANES):
                line = rank[0, pl.ds(row + low // LANES + g, 1), :]
                if factor is not None:
                    line = line * factor
                at = slice(k * size + g * LANES, k * size + (g + 1) * LANES)
                kept = jnp.where(line < own, scores[:, at], jnp.float32(-1.0))
                best = jnp.maximum(best, kept)
                column = jnp.max(kept.reshape(count // 8, 8, LANES), axis=0)
                there = slice(low + g * LANES, low + (g + 1) * LANES)
                acc[slot + k, :, there] = jnp.maximum(acc[slot + k, :, there], column)
        best_ref[...] = best.reshape(best_ref.shape)

    def own_score(h, u=None):
        score(mem.at[1], guest_rank.at[1], guest_acc.at[1], h, u, host_acc, h)

    def up_score(h, u=None):
        score(mem.at[0], guest_rank.at[0], guest_acc.at[0], h, u, host_acc, h)

    def both_score(h, u):
        score(mem.at[0:2], guest_rank, guest_acc, h, u, host_acc, h)

    def part_score(v, h, u=None):
        at = slice(v * unit, (v + 1) * unit)
        score(mem.at[0, at], guest_rank.at[0, at], guest_acc.at[0, at], h, u, host_acc, h)

    def pair_score(h):
        score(pair, pair_rank, pair_acc, h, None, swap_acc, h - 4, sign)

    def two_score(h):
        score(two, two_rank, two_acc, h, None, host_acc, h, slots=2)

    def sweep(f, low, high):
        def body(h, _):
            f(h)
            return 0
        lax.fori_loop(low, high, body, 0)

    def each(f, low, high):
        def body(i, _):
            f(i)
            return 0
        lax.fori_loop(low, high, body, 0)

    with jax.named_scope("own0"):
        own_score(0)
    spread(1, place(x, r), lines, guest_rank.at[0])
    spread(2, place(x, r), lines, pair_rank, sign)
    spread(2, place(1, r) + x * (lines // 2), lines // 2, two_rank)
    with jax.named_scope("core"):
        core_copy(every).wait_recv()
    with jax.named_scope("own1"):
        own_score(1)

    def arrive(p):
        for by_x in (True, False):
            i = 2 * p + (0 if by_x else 1)
            u = i // half

            @if_relay
            def _():
                relay(i)

            with jax.named_scope("y"):
                y_copy(i).wait_recv()
            twin_copy(0, u, cut(i)).start()
            with jax.named_scope("x"):
                x_copy(i).wait_recv()
            twin_copy(1, u, cut(i)).start()
            diag_copy(i, by_x).start()

    def z_wait(u):
        with jax.named_scope("z"):
            z_copy(u, area(u)).wait_recv()

    for u in range(2):
        each(arrive, u * (half // 2), (u + 1) * (half // 2))
        with jax.named_scope("twin"):
            for k in range(2):
                twin_copy(k, u, area(u)).wait_recv()

        @unless_relay
        def _():
            with jax.named_scope("own25"):
                sweep(lambda h: own_score(h, u), 2, 6 - 2 * x)
            if u == 0:
                z_wait(0)
                with jax.named_scope("v0"):
                    sweep(lambda h: part_score(0, h), 0, 2)
            else:
                with jax.named_scope("v0"):
                    sweep(lambda h: part_score(0, h), 2, 6)

                @if_two
                def _():
                    two_copy(0, unit).start()
                z_wait(1)
                with jax.named_scope("v1"):
                    sweep(lambda h: part_score(1, h), 0, 6)

    @if_relay
    def _():
        with jax.named_scope("own25"):
            sweep(own_score, 2, 6 - 2 * x)
        z_wait(0)
        z_wait(1)
        with jax.named_scope("v01"):
            sweep(up_score, 0, 6)

    def lanes(acc):
        return jnp.max(acc[...].T, axis=0, keepdims=True)

    none = jnp.full((1, rows), -1.0, jnp.float32)

    def back_copy(slot):
        target = far_up if slot else device(layer(-1), x, r)
        return send(back_out.at[slot], back_in.at[slot], back_send.at[slot], back_recv.at[slot], target)

    def diag_arrive(i):
        diag_copy(i, True).wait_recv()
        twin_copy(2, i // half, cut(i)).start()

    @if_relay
    def _():
        with jax.named_scope("p45"):
            sweep(pair_score, 4, 6)

    for u in range(2):
        with jax.named_scope("diag"):
            each(diag_arrive, u * half, (u + 1) * half)
            twin_copy(2, u, area(u)).wait_recv()
        with jax.named_scope("last"):
            @pl.when(x == 0)
            def _():
                sweep(lambda h: both_score(h, u), 6, 8)

            @pl.when(x == 1)
            def _():
                sweep(lambda h: up_score(h, u), 6, 8)

    back_out[0, 0:1, :] = none
    back_out[0, 1:2, :] = lanes(guest_acc.at[0])
    back_copy(0).start()

    @if_relay
    def _():
        with jax.named_scope("p67"):
            sweep(pair_score, 6, 8)
            best = lanes(pair_acc)
            back_out[1, 0:1, :] = jnp.where(x == 0, best, none)
            back_out[1, 1:2, :] = jnp.where(x == 0, none, best)
            back_copy(1).start()

    @if_two
    def _():
        with jax.named_scope("two"):
            two_copy(0, unit).wait_recv()
        with jax.named_scope("v2"):
            sweep(lambda k: two_score(4 * x + 2 * k), 0, 2)

    def row_copy(h):
        return send(row_out.at[h - 1], row_in.at[h - 1], row_send, row_sem, peer(h))

    with jax.named_scope("rows"):
        for h in range(7, 0, -1):
            best = jnp.max(host_acc[h], axis=0, keepdims=True)
            other = none
            if h >= 4 and wrap:
                swapped = jnp.max(swap_acc[h - 4], axis=0, keepdims=True)
                other = jnp.where(x == 0, swapped, none)
                best = jnp.where(x == 0, best, jnp.maximum(best, swapped))
            row_out[h - 1, 0:1, :] = best
            row_out[h - 1, 1:2, :] = other
            row_copy(h).start()

    def twob_copy(k):
        return send(two_out, two_in.at[k], twob_send, twob_recv, device(layer(-2), 1, r))

    @if_two
    def _():
        two_out[...] = jnp.broadcast_to(lanes(two_acc), two_out.shape)
        twob_copy(x).start()

    late_ref[...] = jnp.max(host_acc[0], axis=0, keepdims=True)
    early_ref[...] = lanes(guest_acc.at[1])

    def take(best):
        late_ref[...] = jnp.maximum(late_ref[...], best[0:1, :])
        early_ref[...] = jnp.maximum(early_ref[...], best[1:2, :])

    with jax.named_scope("rowin"):
        send(row_out, row_in, row_send, row_sem, peer(1)).wait_recv()
        for h in range(1, 8):
            take(row_in.at[h - 1])
    with jax.named_scope("back"):
        back_copy(0).wait_recv()
        take(back_in.at[0])

        @if_two
        def _():
            @pl.when(x == 1)
            def _():
                send(two_in, two_in, twob_send, twob_recv, far_up).wait_recv()
                for k in range(2):
                    at = slice(k * unit, (k + 1) * unit)
                    early_ref[:, at] = jnp.maximum(early_ref[:, at], two_in[k, 0:1, :])

        if wrap:
            @pl.when(last == 1)
            def _():
                back_copy(1).wait_recv()
                take(back_in.at[1])

    with jax.named_scope("drain"):
        core_copy(every).wait_send()
        x_copy(0, every).wait_send()
        y_copy(0, every).wait_send()
        z_copy(0, every).wait_send()
        diag_copy(0, True, every).wait_send()
        for k in range(3):
            twin_copy(k, 0, every).wait_send()

        @if_two
        def _():
            two_copy(0, unit).wait_send()
            twob_copy(0).wait_send()

        send(row_out, row_in, row_send, row_sem, peer(1)).wait_send()
        back_copy(0).wait_send()

        @if_relay
        def _():
            relay_copy(0, every).wait_send()
            back_copy(1).wait_send()


def shards(embeddings, ranks):
    rows, width = embeddings.shape
    copies = lax.axis_size("rep")
    blocks = lax.axis_size("blk")
    lines = rows // LANES
    dma = pltpu.SemaphoreType.DMA
    vmem = pl.BlockSpec(memory_space=pltpu.VMEM)
    hbm = pl.BlockSpec(memory_space=pltpu.HBM)
    f32, i32, bf16 = jnp.float32, jnp.int32, jnp.bfloat16
    early, late = pl.pallas_call(
        functools.partial(kernel, blocks, copies),
        out_shape=[jax.ShapeDtypeStruct((1, rows), f32)] * 2,
        in_specs=[hbm, hbm],
        out_specs=[vmem, vmem],
        scratch_shapes=[
            pltpu.VMEM((rows, width), f32),
            pltpu.VMEM((3, 2 * copies * lines, LANES), i32),
            pltpu.VMEM((9, rows, width), bf16),
            pltpu.VMEM((rows, width), bf16),
            pltpu.VMEM((rows // 2, width), bf16),
            pltpu.VMEM((2, rows, LANES), i32),
            pltpu.VMEM((rows, LANES), i32),
            pltpu.VMEM((rows // 2, LANES), i32),
            pltpu.VMEM((2, rows, LANES), f32),
            pltpu.VMEM((rows, LANES), f32),
            pltpu.VMEM((rows // 2, LANES), f32),
            pltpu.VMEM((8, 8, rows), f32),
            pltpu.VMEM((4, 8, rows), f32),
            pltpu.VMEM((7, 2, rows), f32),
            pltpu.VMEM((7, 2, rows), f32),
            pltpu.VMEM((2, 2, rows), f32),
            pltpu.VMEM((2, 2, rows), f32),
            pltpu.VMEM((2, rows // 2), f32),
            pltpu.VMEM((2, 2, rows // 2), f32),
            dma((CHUNKS,)), dma,
            dma, dma, dma, dma((CHUNKS,)), dma, dma((CHUNKS,)), dma, dma((2,)), dma((2 * CHUNKS,)),
            dma, dma, dma((CHUNKS,)), dma((3,)), dma((3, 2)), dma, dma,
            dma, dma, dma((2,)), dma((2,)), dma, dma,
        ],
        compiler_params=pltpu.CompilerParams(
            collective_id=0, has_side_effects=True, vmem_limit_bytes=56_500_000
        ),
    )(embeddings, ranks.reshape(-1, LANES))
    return early.reshape(rows), late.reshape(rows)


def solution(mesh):
    return jax.shard_map(
        shards,
        mesh=mesh,
        in_specs=(P(("blk", "rep"), None), P()),
        out_specs=(P(("blk", "rep")), P(("blk", "rep"))),
        check_vma=False,
    )
```

```python
import functools

import jax
import jax.numpy as jnp
from jax import lax
from jax.experimental import pallas as pl
from jax.experimental.pallas import tpu as pltpu
from jax.sharding import PartitionSpec as P

CHUNKS = 8
LANES = 128
MESH = pl.DeviceIdType.MESH


def kernel(
    blocks, copies, emb_hbm, ranks_hbm, out_ref,
    emb, rank, mem, pair, two,
    guest_rank, pair_rank, two_rank, guest_acc, pair_acc, two_acc, host_acc, swap_acc,
    row_out, row_in, back_out, back_in, two_out, two_in,
    emb_sem, rank_sem,
    core_send, core_recv, x_send, x_recv, y_send, y_recv, z_send, z_recv, pair_recv,
    relay_send, diag_send, diag_recv, twin_send, twin_recv, two_send, two_recv,
    row_send, row_sem, back_send, back_recv, twob_send, twob_recv,
):
    rows = emb.shape[0]
    early_ref, late_ref = out_ref.at[0:1], out_ref.at[1:2]
    part = rows // CHUNKS
    unit = rows // 2
    small = part // 2
    half = CHUNKS // 2
    lines = rows // LANES
    layers = blocks // 2
    wrap = layers == 4

    b = blocks - 1 - lax.axis_index("blk")
    r = lax.axis_index("rep")
    x = lax.rem(b, 2)
    l = b // 2

    def flip_rep(k):
        dy, dc = k // 2, k % 2
        y, c = r // 2, lax.rem(r, 2)
        return 2 * (y + dy - 2 * y * dy) + c + dc - 2 * c * dc

    def flip_x(d):
        return x + d - 2 * x * d

    def device(row, column, copy):
        return (blocks - 1 - 2 * row - column, copy)

    def peer(h):
        return device(l, flip_x(h // 4), flip_rep(h % 4))

    def layer(offset):
        return lax.rem(l + offset + layers, layers)

    if wrap:
        last = l // (layers - 1)
        is_relay = l == 1
        has_two = lax.rem(l, 2) == 0
        two_turn = l // 2
    else:
        last = 0 * l
        is_relay = None
        has_two = None
        two_turn = 0 * l

    def if_relay(f):
        if wrap:
            pl.when(is_relay)(f)

    def unless_relay(f):
        if wrap:
            pl.when(l != 1)(f)
        else:
            f()

    def if_two(f):
        if wrap:
            pl.when(has_two)(f)
        else:
            f()

    up = device(layer(1), x, r)
    down = device(layer(-1), x, r)
    far_up = device(layer(2), x, r)
    far_down = device(layer(-2), x, r)

    def cut(i):
        return pl.ds(pl.multiple_of(i * part, part), part)

    def emb_copy(i):
        return pltpu.make_async_copy(emb_hbm.at[cut(i)], emb.at[cut(i)], emb_sem.at[i])

    def rank_copy(k):
        size = 2 * copies * lines
        return pltpu.make_async_copy(
            ranks_hbm.at[pl.ds(pl.multiple_of((layers - 1 - layer(-k)) * size, size), size)],
            rank.at[k], rank_sem,
        )

    barrier = pltpu.get_barrier_semaphore()

    def greet(target):
        pl.semaphore_signal(barrier, inc=1, device_id=target, device_id_type=MESH)

    for h in (1, 2, 4):
        greet(peer(h))
    if wrap:
        @pl.when(l == 0)
        def _():
            greet(device(l + 1, x, r))

        @pl.when(l > 0)
        def _():
            greet(down)

        @pl.when(l < layers - 1)
        def _():
            greet(far_up)
        expected = 5 - last
    else:
        greet(down)
        greet(far_down)
        expected = 5

    for i in range(CHUNKS):
        emb_copy(i).start()
    for k in range(3):
        rank_copy(k).start()

    def send(src, dst, send_sem, recv_sem, device):
        return pltpu.make_async_remote_copy(
            src_ref=src, dst_ref=dst, send_sem=send_sem, recv_sem=recv_sem,
            device_id=device, device_id_type=MESH,
        )

    def host(h):
        return mem.at[h + 1]

    def area(u):
        return pl.ds(pl.multiple_of(u * unit, unit), unit)

    every = pl.ds(0, rows)

    def core_copy(at):
        return send(host(0).at[at], host(1).at[at], core_send, core_recv, peer(1))

    def x_copy(i, at=None):
        at = cut(i) if at is None else at
        return send(host(0).at[at], host(4).at[at], x_send, x_recv.at[i], peer(4))

    def y_copy(i, at=None):
        at = cut(i) if at is None else at
        return send(host(0).at[at], host(2).at[at], y_send, y_recv.at[i], peer(2))

    def z_copy(u, at):
        return send(host(0).at[at], mem.at[0, at], z_send, z_recv.at[u], up)

    def far_copy(k, at):
        return send(host(0).at[at], pair.at[at], z_send, pair_recv.at[k], far_down)

    def relay_copy(u, at):
        return send(pair.at[at], mem.at[0, at], relay_send, z_recv.at[u], down)

    def diag_copy(i, by_x, at=None):
        at = cut(i) if at is None else at
        source, target = (2, peer(4)) if by_x else (4, peer(2))
        return send(host(source).at[at], host(6).at[at], diag_send, diag_recv.at[i], target)

    def twin_copy(k, u, at):
        slot = 2 + 2 * k
        return send(
            host(slot).at[at], host(slot + 1).at[at], twin_send.at[k], twin_recv.at[k, u], peer(1)
        )

    def two_copy(i, size):
        at = pl.ds(pl.multiple_of(x * unit + i * part, part), size)
        there = pl.ds(i * part, size)
        return send(host(4 * (1 - x)).at[at], two.at[there], two_send, two_recv, far_up)

    def normalise(i):
        emb_copy(i).wait()
        v = emb[cut(i), :]
        squares = jnp.sum(v * v, axis=1, keepdims=True)
        mem[1, cut(i), :] = (v * lax.rsqrt(squares + 1e-06)).astype(jnp.bfloat16)

    def piece(k):
        return pl.ds(pl.multiple_of(k * small, small), small)

    def ascend(i):
        def far():
            for n in range(part // small):
                k = i * (part // small) + n
                far_copy(k, piece(k)).start()

        if wrap:
            pl.when(last == 1)(far)

            @pl.when(last == 0)
            def _():
                z_copy(i // half, cut(i)).start()
        else:
            z_copy(i // half, cut(i)).start()

    def launch(i):
        ascend(i)
        x_copy(i).start()
        y_copy(i).start()
        core_copy(cut(i)).start()

    with jax.named_scope("norm"):
        normalise(0)
        normalise(1)
    with jax.named_scope("barrier"):
        pl.semaphore_wait(barrier, expected)

    def prepare(i, _):
        launch(i - 2)
        normalise(i)
        return 0

    with jax.named_scope("prepare"):
        launch(0)
        normalise(2)
        lax.fori_loop(3, CHUNKS, prepare, 0)
        for k in range(3):
            rank_copy(k).wait()
        launch(CHUNKS - 2)
        launch(CHUNKS - 1)

    def relay(i):
        for n in range(part // small):
            k = i * (part // small) + n
            with jax.named_scope("w"):
                far_copy(k, piece(k)).wait_recv()
            relay_copy(i // half, piece(k)).start()

    sign = 2 * x - 1

    def place(column, copy):
        return (copies * (1 - column) + copy) * lines

    def spread(slot, row, count, out, factor=None):
        for g in range(count):
            line = rank[slot, pl.ds(row + g, 1), :]
            if factor is not None:
                line = line * factor
            out[g * LANES:(g + 1) * LANES, :] = jnp.broadcast_to(line, (LANES, LANES)).T

    spread(0, place(x, r), lines, guest_rank.at[1])
    for acc in (guest_acc, pair_acc, two_acc, host_acc, swap_acc):
        acc[...] = jnp.full(acc.shape, -1.0, jnp.float32)

    def score(guest, guest_line, best_ref, h, u, acc, slot, factor=None, slots=1):
        if u is None:
            low, size = 0, rows
            hosts = mem[pl.ds(h + 1, slots)].reshape(slots * rows, mem.shape[2])
        else:
            low, size = u * unit, unit
            hosts = mem[h + 1, area(u), :]
        count = guest_line.size // LANES
        lhs = guest[...].reshape(count, hosts.shape[1])
        scores = lax.dot_general(
            lhs, hosts, (((1,), (1,)), ((), ())), preferred_element_type=jnp.float32
        )
        own = guest_line[...].reshape(count, LANES)
        best = best_ref[...].reshape(count, LANES)
        for k in range(slots):
            row = place(flip_x((h + k) // 4), flip_rep((h + k) % 4))
            for g in range(size // LANES):
                line = rank[0, pl.ds(row + low // LANES + g, 1), :]
                if factor is not None:
                    line = line * factor
                at = slice(k * size + g * LANES, k * size + (g + 1) * LANES)
                kept = jnp.where(line < own, scores[:, at], jnp.float32(-1.0))
                best = jnp.maximum(best, kept)
                column = jnp.max(kept.reshape(count // 8, 8, LANES), axis=0)
                there = pl.ds(pl.multiple_of(low + g * LANES, LANES), LANES)
                acc[slot + k, :, there] = jnp.maximum(acc[slot + k, :, there], column)
        best_ref[...] = best.reshape(best_ref.shape)

    def own_score(h, u=None):
        score(mem.at[1], guest_rank.at[1], guest_acc.at[1], h, u, host_acc, h)

    def up_score(h, u=None):
        score(mem.at[0], guest_rank.at[0], guest_acc.at[0], h, u, host_acc, h)

    def both_score(h, u):
        score(mem.at[0:2], guest_rank, guest_acc, h, u, host_acc, h)

    def part_score(v, h, u=None):
        at = slice(v * unit, (v + 1) * unit)
        score(mem.at[0, at], guest_rank.at[0, at], guest_acc.at[0, at], h, u, host_acc, h)

    def pair_score(h):
        score(pair, pair_rank, pair_acc, h, None, swap_acc, h - 4, sign)

    def two_score(h):
        score(two, two_rank, two_acc, h, None, host_acc, h, slots=2)

    def sweep(f, low, high):
        def body(h, _):
            f(h)
            return 0
        lax.fori_loop(low, high, body, 0)

    def each(f, low, high):
        def body(i, _):
            f(i)
            return 0
        lax.fori_loop(low, high, body, 0)

    with jax.named_scope("own0"):
        own_score(0)
    spread(1, place(x, r), lines, guest_rank.at[0])
    spread(2, place(x, r), lines, pair_rank, sign)
    spread(2, place(1, r) + x * (lines // 2), lines // 2, two_rank)
    with jax.named_scope("core"):
        core_copy(every).wait_recv()
    with jax.named_scope("own1"):
        own_score(1)

    def arrive(p, u):
        for by_x in (True, False):
            i = 2 * p + (0 if by_x else 1)

            @if_relay
            def _():
                relay(i)
                if u == 1:
                    k = i - half

                    @pl.when(k < 4 - 2 * x)
                    def _():
                        own_score(2 + k, 0)

                    @pl.when(k < 2)
                    def _():
                        part_score(0, k)

            with jax.named_scope("y"):
                y_copy(i).wait_recv()
            twin_copy(0, u, cut(i)).start()
            with jax.named_scope("x"):
                x_copy(i).wait_recv()
            twin_copy(1, u, cut(i)).start()
            diag_copy(i, by_x).start()

    def two_post(u):
        @if_two
        def _():
            @pl.when(two_turn == u)
            def _():
                two_copy(0, unit).start()

    def z_wait(u):
        with jax.named_scope("z"):
            z_copy(u, area(u)).wait_recv()

    for u in range(2):
        each(lambda p: arrive(p, u), u * (half // 2), (u + 1) * (half // 2))
        with jax.named_scope("twin"):
            for k in range(2):
                twin_copy(k, u, area(u)).wait_recv()

        if u == 0:
            two_post(0)

            @unless_relay
            def _():
                with jax.named_scope("own25"):
                    sweep(lambda h: own_score(h, 0), 2, 6 - 2 * x)
                z_wait(0)
                with jax.named_scope("v0"):
                    sweep(lambda h: part_score(0, h), 0, 2)

            @if_relay
            def _():
                z_wait(0)

    def diag_arrive(i):
        diag_copy(i, True).wait_recv()
        twin_copy(2, i // half, cut(i)).start()

    with jax.named_scope("own25"):
        sweep(lambda h: own_score(h, 1), 2, 6 - 2 * x)
    with jax.named_scope("v0"):
        sweep(lambda h: part_score(0, h), 2, 2 + 2 * x)
        two_post(1)
        sweep(lambda h: part_score(0, h), 2 + 2 * x, 6)
    z_wait(1)

    def later(h):
        @pl.when(h == 3)
        def _():
            with jax.named_scope("diag"):
                each(diag_arrive, 0, half)
        part_score(1, h)

    with jax.named_scope("v1"):
        sweep(later, 0, 6)

    def lanes(acc):
        return jnp.max(acc[...].T, axis=0, keepdims=True)

    none = jnp.full((1, rows), -1.0, jnp.float32)

    def back_copy(slot):
        target = far_up if slot else device(layer(-1), x, r)
        return send(back_out.at[slot], back_in.at[slot], back_send.at[slot], back_recv.at[slot], target)

    @if_relay
    def _():
        with jax.named_scope("p45"):
            sweep(pair_score, 4, 6)

    def last_score(t):
        u, odd = t // 2, lax.rem(t, 2)

        @pl.when(t == 2)
        def _():
            with jax.named_scope("diag"):
                each(diag_arrive, half, CHUNKS)

        @pl.when(odd == 1)
        def _():
            with jax.named_scope("twin2"):
                twin_copy(2, u, area(u)).wait_recv()

        @pl.when(x == 0)
        def _():
            both_score(6 + odd, u)

        @pl.when(x == 1)
        def _():
            up_score(6 + odd, u)

    with jax.named_scope("last"):
        each(last_score, 0, 4)

    back_out[0, 0:1, :] = none
    back_out[0, 1:2, :] = lanes(guest_acc.at[0])
    back_copy(0).start()

    @if_relay
    def _():
        with jax.named_scope("p67"):
            sweep(pair_score, 6, 8)
            best = lanes(pair_acc)
            back_out[1, 0:1, :] = jnp.where(x == 0, best, none)
            back_out[1, 1:2, :] = jnp.where(x == 0, none, best)
            back_copy(1).start()

    def row_copy(h):
        return send(row_out.at[h - 1], row_in.at[h - 1], row_send, row_sem, peer(h))

    def row_post(h):
        row_out[h - 1, 0:1, :] = jnp.max(host_acc[h], axis=0, keepdims=True)
        row_out[h - 1, 1:2, :] = none
        row_copy(h).start()

    @unless_relay
    def _():
        sweep(row_post, 4 - 3 * x, 8 - 4 * x)

    def row_merge(h):
        best = jnp.max(host_acc[h], axis=0, keepdims=True)
        swapped = jnp.max(swap_acc[h - 4], axis=0, keepdims=True)
        row_out[h - 1, 0:1, :] = jnp.where(x == 0, best, jnp.maximum(best, swapped))
        row_out[h - 1, 1:2, :] = jnp.where(x == 0, swapped, none)
        row_copy(h).start()

    @if_relay
    def _():
        sweep(row_merge, 4, 8)
        sweep(row_post, 1, 4)

    @if_two
    def _():
        with jax.named_scope("two"):
            two_copy(0, unit).wait_recv()
        with jax.named_scope("v2"):
            sweep(lambda k: two_score(4 * x + 2 * k), 0, 2)

    with jax.named_scope("rows"):
        @unless_relay
        def _():
            sweep(row_post, 1 + 3 * x, 4 + 4 * x)

    def twob_copy(k):
        return send(two_out, two_in.at[k], twob_send, twob_recv, device(layer(-2), 1, r))

    @if_two
    def _():
        two_out[...] = jnp.broadcast_to(lanes(two_acc), two_out.shape)
        twob_copy(x).start()

    late_ref[...] = jnp.max(host_acc[0], axis=0, keepdims=True)
    early_ref[...] = lanes(guest_acc.at[1])

    def take(best):
        late_ref[...] = jnp.maximum(late_ref[...], best[0:1, :])
        early_ref[...] = jnp.maximum(early_ref[...], best[1:2, :])

    with jax.named_scope("rowin"):
        send(row_out, row_in, row_send, row_sem, peer(1)).wait_recv()
        for h in range(1, 8):
            take(row_in.at[h - 1])
    with jax.named_scope("back"):
        back_copy(0).wait_recv()
        take(back_in.at[0])

        @if_two
        def _():
            @pl.when(x == 1)
            def _():
                send(two_in, two_in, twob_send, twob_recv, far_up).wait_recv()
                for k in range(2):
                    at = slice(k * unit, (k + 1) * unit)
                    early_ref[:, at] = jnp.maximum(early_ref[:, at], two_in[k, 0:1, :])

        if wrap:
            @pl.when(last == 1)
            def _():
                back_copy(1).wait_recv()
                take(back_in.at[1])

    with jax.named_scope("drain"):
        core_copy(every).wait_send()
        x_copy(0, every).wait_send()
        y_copy(0, every).wait_send()
        z_copy(0, every).wait_send()
        diag_copy(0, True, every).wait_send()
        for k in range(3):
            twin_copy(k, 0, every).wait_send()

        @if_two
        def _():
            two_copy(0, unit).wait_send()
            twob_copy(0).wait_send()

        send(row_out, row_in, row_send, row_sem, peer(1)).wait_send()
        back_copy(0).wait_send()

        @if_relay
        def _():
            relay_copy(0, every).wait_send()
            back_copy(1).wait_send()


def shards(embeddings, ranks):
    rows, width = embeddings.shape
    copies = lax.axis_size("rep")
    blocks = lax.axis_size("blk")
    lines = rows // LANES
    dma = pltpu.SemaphoreType.DMA
    vmem = pl.BlockSpec(memory_space=pltpu.VMEM)
    hbm = pl.BlockSpec(memory_space=pltpu.HBM)
    f32, i32, bf16 = jnp.float32, jnp.int32, jnp.bfloat16
    both = pl.pallas_call(
        functools.partial(kernel, blocks, copies),
        out_shape=jax.ShapeDtypeStruct((2, rows), f32),
        in_specs=[hbm, hbm],
        out_specs=vmem,
        scratch_shapes=[
            pltpu.VMEM((rows, width), f32),
            pltpu.VMEM((3, 2 * copies * lines, LANES), i32),
            pltpu.VMEM((9, rows, width), bf16),
            pltpu.VMEM((rows, width), bf16),
            pltpu.VMEM((rows // 2, width), bf16),
            pltpu.VMEM((2, rows, LANES), i32),
            pltpu.VMEM((rows, LANES), i32),
            pltpu.VMEM((rows // 2, LANES), i32),
            pltpu.VMEM((2, rows, LANES), f32),
            pltpu.VMEM((rows, LANES), f32),
            pltpu.VMEM((rows // 2, LANES), f32),
            pltpu.VMEM((8, 8, rows), f32),
            pltpu.VMEM((4, 8, rows), f32),
            pltpu.VMEM((7, 2, rows), f32),
            pltpu.VMEM((7, 2, rows), f32),
            pltpu.VMEM((2, 2, rows), f32),
            pltpu.VMEM((2, 2, rows), f32),
            pltpu.VMEM((2, rows // 2), f32),
            pltpu.VMEM((2, 2, rows // 2), f32),
            dma((CHUNKS,)), dma,
            dma, dma, dma, dma((CHUNKS,)), dma, dma((CHUNKS,)), dma, dma((2,)), dma((2 * CHUNKS,)),
            dma, dma, dma((CHUNKS,)), dma((3,)), dma((3, 2)), dma, dma,
            dma, dma, dma((2,)), dma((2,)), dma, dma,
        ],
        compiler_params=pltpu.CompilerParams(
            collective_id=0, has_side_effects=True, vmem_limit_bytes=56_500_000
        ),
    )(embeddings, ranks.reshape(-1, LANES))
    return both[0], both[1]


def solution(mesh):
    return jax.shard_map(
        shards,
        mesh=mesh,
        in_specs=(P(("blk", "rep"), None), P()),
        out_specs=(P(("blk", "rep")), P(("blk", "rep"))),
        check_vma=False,
    )
```

```python
import functools

import jax
import jax.numpy as jnp
from jax import lax
from jax.experimental import pallas as pl
from jax.experimental.pallas import tpu as pltpu
from jax.sharding import PartitionSpec as P

CHUNKS = 8
LANES = 128
MESH = pl.DeviceIdType.MESH


def program(
    blocks, copies, emb_hbm, ranks_hbm, out_ref,
    emb, rank, mem, pair, two,
    guest_rank, pair_rank, two_rank, guest_acc, pair_acc, two_acc, host_acc, swap_acc,
    row_out, row_in, back_out, back_in, two_out, two_in,
    emb_sem, rank_sem,
    core_send, core_recv, x_send, x_recv, y_send, y_recv, z_send, z_recv, pair_recv,
    relay_send, diag_send, diag_recv, twin_send, twin_recv, two_send, two_recv,
    row_send, row_sem, back_send, back_recv, twob_send, twob_recv,
):
    rows = emb.shape[0]
    early_ref, late_ref = out_ref.at[0:1], out_ref.at[1:2]
    part = rows // CHUNKS
    unit = rows // 2
    small = part // 2
    half = CHUNKS // 2
    lines = rows // LANES
    layers = blocks // 2
    wrap = layers == 4

    b = blocks - 1 - lax.axis_index("blk")
    r = lax.axis_index("rep")
    x = lax.rem(b, 2)
    l = b // 2

    def flip_rep(k):
        dy, dc = k // 2, k % 2
        y, c = r // 2, lax.rem(r, 2)
        return 2 * (y + dy - 2 * y * dy) + c + dc - 2 * c * dc

    def flip_x(d):
        return x + d - 2 * x * d

    def device(row, column, copy):
        return (blocks - 1 - 2 * row - column, copy)

    def peer(h):
        return device(l, flip_x(h // 4), flip_rep(h % 4))

    def layer(offset):
        return lax.rem(l + offset + layers, layers)

    if wrap:
        last = l // (layers - 1)
        is_relay = l == 1
        has_two = lax.rem(l, 2) == 0
        two_turn = l // 2
    else:
        last = 0 * l
        is_relay = None
        has_two = None
        two_turn = 0 * l

    def if_relay(f):
        if wrap:
            pl.when(is_relay)(f)

    def unless_relay(f):
        if wrap:
            pl.when(l != 1)(f)
        else:
            f()

    def if_two(f):
        if wrap:
            pl.when(has_two)(f)
        else:
            f()

    up = device(layer(1), x, r)
    down = device(layer(-1), x, r)
    far_up = device(layer(2), x, r)
    far_down = device(layer(-2), x, r)

    def cut(i):
        return pl.ds(pl.multiple_of(i * part, part), part)

    def emb_copy(i):
        return pltpu.make_async_copy(emb_hbm.at[cut(i)], emb.at[cut(i)], emb_sem.at[i])

    def rank_copy(k):
        size = 2 * copies * lines
        return pltpu.make_async_copy(
            ranks_hbm.at[pl.ds(pl.multiple_of((layers - 1 - layer(-k)) * size, size), size)],
            rank.at[k], rank_sem,
        )

    barrier = pltpu.get_barrier_semaphore()

    def greet(target):
        pl.semaphore_signal(barrier, inc=1, device_id=target, device_id_type=MESH)

    for h in (1, 2, 4):
        greet(peer(h))
    if wrap:
        @pl.when(l == 0)
        def _():
            greet(device(l + 1, x, r))

        @pl.when(l > 0)
        def _():
            greet(down)

        @pl.when(l < layers - 1)
        def _():
            greet(far_up)
        expected = 5 - last
    else:
        greet(down)
        greet(far_down)
        expected = 5

    for i in range(CHUNKS):
        emb_copy(i).start()
    for k in range(3):
        rank_copy(k).start()

    def send(src, dst, send_sem, recv_sem, device):
        return pltpu.make_async_remote_copy(
            src_ref=src, dst_ref=dst, send_sem=send_sem, recv_sem=recv_sem,
            device_id=device, device_id_type=MESH,
        )

    def host(h):
        return mem.at[h + 1]

    def area(u):
        return pl.ds(pl.multiple_of(u * unit, unit), unit)

    every = pl.ds(0, rows)

    def core_copy(at):
        return send(host(0).at[at], host(1).at[at], core_send, core_recv, peer(1))

    def x_copy(i, at=None):
        at = cut(i) if at is None else at
        return send(host(0).at[at], host(4).at[at], x_send, x_recv.at[i], peer(4))

    def y_copy(i, at=None):
        at = cut(i) if at is None else at
        return send(host(0).at[at], host(2).at[at], y_send, y_recv.at[i], peer(2))

    def z_copy(u, at):
        return send(host(0).at[at], mem.at[0, at], z_send, z_recv.at[u], up)

    def far_copy(k, at):
        return send(host(0).at[at], pair.at[at], z_send, pair_recv.at[k], far_down)

    def relay_copy(u, at):
        return send(pair.at[at], mem.at[0, at], relay_send, z_recv.at[u], down)

    def diag_copy(i, by_x, at=None):
        at = cut(i) if at is None else at
        source, target = (2, peer(4)) if by_x else (4, peer(2))
        return send(host(source).at[at], host(6).at[at], diag_send, diag_recv.at[i], target)

    def twin_copy(k, u, at):
        slot = 2 + 2 * k
        return send(
            host(slot).at[at], host(slot + 1).at[at], twin_send.at[k], twin_recv.at[k, u], peer(1)
        )

    def two_copy(i, size):
        at = pl.ds(pl.multiple_of(x * unit + i * part, part), size)
        there = pl.ds(i * part, size)
        return send(host(4 * (1 - x)).at[at], two.at[there], two_send, two_recv, far_up)

    def normalise(i):
        emb_copy(i).wait()
        v = emb[cut(i), :]
        squares = jnp.sum(v * v, axis=1, keepdims=True)
        mem[1, cut(i), :] = (v * lax.rsqrt(squares + 1e-06)).astype(jnp.bfloat16)

    def piece(k):
        return pl.ds(pl.multiple_of(k * small, small), small)

    def ascend(i):
        def far():
            for n in range(part // small):
                k = i * (part // small) + n
                far_copy(k, piece(k)).start()

        if wrap:
            pl.when(last == 1)(far)

            @pl.when(last == 0)
            def _():
                z_copy(i // half, cut(i)).start()
        else:
            z_copy(i // half, cut(i)).start()

    def launch(i):
        ascend(i)
        x_copy(i).start()
        y_copy(i).start()
        core_copy(cut(i)).start()

    with jax.named_scope("norm"):
        normalise(0)
        normalise(1)
    with jax.named_scope("barrier"):
        pl.semaphore_wait(barrier, expected)

    def prepare(i, _):
        launch(i - 2)
        normalise(i)
        return 0

    with jax.named_scope("prepare"):
        launch(0)
        normalise(2)
        lax.fori_loop(3, CHUNKS, prepare, 0)
        for k in range(3):
            rank_copy(k).wait()
        launch(CHUNKS - 2)
        launch(CHUNKS - 1)

    def relay(i):
        for n in range(part // small):
            k = i * (part // small) + n
            with jax.named_scope("w"):
                far_copy(k, piece(k)).wait_recv()
            relay_copy(i // half, piece(k)).start()

    sign = 2 * x - 1

    def place(column, copy):
        return (copies * (1 - column) + copy) * lines

    def spread(slot, row, count, out, factor=None):
        for g in range(count):
            line = rank[slot, pl.ds(row + g, 1), :]
            if factor is not None:
                line = line * factor
            out[g * LANES:(g + 1) * LANES, :] = jnp.broadcast_to(line, (LANES, LANES)).T

    spread(0, place(x, r), lines, guest_rank.at[1])
    for acc in (guest_acc, pair_acc, two_acc, host_acc, swap_acc):
        acc[...] = jnp.full(acc.shape, -1.0, jnp.float32)

    def score(guest, guest_line, best_ref, h, u, acc, slot, factor=None, slots=1):
        if u is None:
            low, size = 0, rows
            hosts = mem[pl.ds(h + 1, slots)].reshape(slots * rows, mem.shape[2])
        else:
            low, size = u * unit, unit
            hosts = mem[h + 1, area(u), :]
        count = guest_line.size // LANES
        lhs = guest[...].reshape(count, hosts.shape[1])
        scores = lax.dot_general(
            lhs, hosts, (((1,), (1,)), ((), ())), preferred_element_type=jnp.float32
        )
        own = guest_line[...].reshape(count, LANES)
        best = best_ref[...].reshape(count, LANES)
        for k in range(slots):
            row = place(flip_x((h + k) // 4), flip_rep((h + k) % 4))
            for g in range(size // LANES):
                line = rank[0, pl.ds(row + low // LANES + g, 1), :]
                if factor is not None:
                    line = line * factor
                at = slice(k * size + g * LANES, k * size + (g + 1) * LANES)
                kept = jnp.where(line < own, scores[:, at], jnp.float32(-1.0))
                best = jnp.maximum(best, kept)
                column = jnp.max(kept.reshape(count // 8, 8, LANES), axis=0)
                there = pl.ds(pl.multiple_of(low + g * LANES, LANES), LANES)
                acc[slot + k, :, there] = jnp.maximum(acc[slot + k, :, there], column)
        best_ref[...] = best.reshape(best_ref.shape)

    def own_score(h, u=None):
        score(mem.at[1], guest_rank.at[1], guest_acc.at[1], h, u, host_acc, h)

    def up_score(h, u=None):
        score(mem.at[0], guest_rank.at[0], guest_acc.at[0], h, u, host_acc, h)

    def both_score(h, u):
        score(mem.at[0:2], guest_rank, guest_acc, h, u, host_acc, h)

    def part_score(v, h, u=None):
        at = slice(v * unit, (v + 1) * unit)
        score(mem.at[0, at], guest_rank.at[0, at], guest_acc.at[0, at], h, u, host_acc, h)

    def pair_score(h):
        score(pair, pair_rank, pair_acc, h, None, swap_acc, h - 4, sign)

    def two_score(h):
        score(two, two_rank, two_acc, h, None, host_acc, h, slots=4)

    def sweep(f, low, high):
        def body(h, _):
            f(h)
            return 0
        lax.fori_loop(low, high, body, 0)

    def each(f, low, high):
        def body(i, _):
            f(i)
            return 0
        lax.fori_loop(low, high, body, 0)

    with jax.named_scope("own0"):
        own_score(0)
    spread(1, place(x, r), lines, guest_rank.at[0])
    spread(2, place(x, r), lines, pair_rank, sign)
    spread(2, place(1, r) + x * (lines // 2), lines // 2, two_rank)
    with jax.named_scope("core"):
        core_copy(every).wait_recv()
    with jax.named_scope("own1"):
        own_score(1)

    def arrive(p, u):
        for by_x in (True, False):
            i = 2 * p + (0 if by_x else 1)

            @if_relay
            def _():
                relay(i)
                if u == 1:
                    k = i - half

                    @pl.when(k < 4 - 2 * x)
                    def _():
                        own_score(2 + k, 0)

                    @pl.when(k < 2)
                    def _():
                        part_score(0, k)

            with jax.named_scope("y"):
                y_copy(i).wait_recv()
            twin_copy(0, u, cut(i)).start()
            with jax.named_scope("x"):
                x_copy(i).wait_recv()
            twin_copy(1, u, cut(i)).start()
            diag_copy(i, by_x).start()

    def two_post(u):
        @if_two
        def _():
            @pl.when(two_turn == u)
            def _():
                two_copy(0, unit).start()

    def z_wait(u):
        with jax.named_scope("z"):
            z_copy(u, area(u)).wait_recv()

    for u in range(2):
        each(lambda p: arrive(p, u), u * (half // 2), (u + 1) * (half // 2))
        with jax.named_scope("twin"):
            for k in range(2):
                twin_copy(k, u, area(u)).wait_recv()

        if u == 0:
            two_post(0)

            @unless_relay
            def _():
                with jax.named_scope("own25"):
                    sweep(lambda h: own_score(h, 0), 2, 6 - 2 * x)
                z_wait(0)
                with jax.named_scope("v0"):
                    sweep(lambda h: part_score(0, h), 0, 2)

            @if_relay
            def _():
                z_wait(0)

    def diag_arrive(i):
        diag_copy(i, True).wait_recv()
        twin_copy(2, i // half, cut(i)).start()

    with jax.named_scope("own25"):
        sweep(lambda h: own_score(h, 1), 2, 5 - x)
        two_post(1)
        sweep(lambda h: own_score(h, 1), 5 - x, 6 - 2 * x)
    with jax.named_scope("v0"):
        sweep(lambda h: part_score(0, h), 2, 6)
    z_wait(1)

    def later(h):
        for turn, low in ((0, 0), (2, 2), (5, half)):
            @pl.when(h == turn)
            def _():
                with jax.named_scope("diag"):
                    each(diag_arrive, low, low + 2)
        part_score(1, h)

    with jax.named_scope("v1"):
        sweep(later, 0, 6)

    def lanes(acc):
        return jnp.max(acc[...].T, axis=0, keepdims=True)

    none = jnp.full((1, rows), -1.0, jnp.float32)

    def back_copy(slot):
        target = far_up if slot else device(layer(-1), x, r)
        return send(back_out.at[slot], back_in.at[slot], back_send.at[slot], back_recv.at[slot], target)

    def last_score(t):
        u, odd = t // 2, lax.rem(t, 2)

        @pl.when(t == 1)
        def _():
            with jax.named_scope("diag"):
                each(diag_arrive, half + 2, CHUNKS)

        @pl.when(odd == 1)
        def _():
            with jax.named_scope("twin2"):
                twin_copy(2, u, area(u)).wait_recv()

        @pl.when(x == 0)
        def _():
            both_score(6 + odd, u)

        @pl.when(x == 1)
        def _():
            up_score(6 + odd, u)

        @if_relay
        def _():
            with jax.named_scope("pair"):
                pair_score(4 + t)

    with jax.named_scope("last"):
        each(last_score, 0, 4)

    @if_relay
    def _():
        best = lanes(pair_acc)
        back_out[1, 0:1, :] = jnp.where(x == 0, best, none)
        back_out[1, 1:2, :] = jnp.where(x == 0, none, best)
        back_copy(1).start()

    back_out[0, 0:1, :] = none
    back_out[0, 1:2, :] = lanes(guest_acc.at[0])
    back_copy(0).start()

    def twob_copy(k):
        return send(two_out, two_in.at[k], twob_send, twob_recv, device(layer(-2), 1, r))

    def row_copy(h):
        return send(row_out.at[h - 1], row_in.at[h - 1], row_send, row_sem, peer(h))

    def row_post(h):
        row_out[h - 1, 0:1, :] = jnp.max(host_acc[h], axis=0, keepdims=True)
        row_out[h - 1, 1:2, :] = none
        row_copy(h).start()

    @unless_relay
    def _():
        sweep(row_post, 4 - 3 * x, 8 - 4 * x)

    def row_merge(h):
        best = jnp.max(host_acc[h], axis=0, keepdims=True)
        swapped = jnp.max(swap_acc[h - 4], axis=0, keepdims=True)
        row_out[h - 1, 0:1, :] = jnp.where(x == 0, best, jnp.maximum(best, swapped))
        row_out[h - 1, 1:2, :] = jnp.where(x == 0, swapped, none)
        row_copy(h).start()

    @if_relay
    def _():
        sweep(row_merge, 4, 8)
        sweep(row_post, 1, 4)

    @if_two
    def _():
        with jax.named_scope("two"):
            two_copy(0, unit).wait_recv()
        with jax.named_scope("v2"):
            two_score(4 * x)
        two_out[...] = jnp.broadcast_to(lanes(two_acc), two_out.shape)
        twob_copy(x).start()

    with jax.named_scope("rows"):
        @unless_relay
        def _():
            sweep(row_post, 1 + 3 * x, 4 + 4 * x)

    late_ref[...] = jnp.max(host_acc[0], axis=0, keepdims=True)
    early_ref[...] = lanes(guest_acc.at[1])

    def take(best):
        late_ref[...] = jnp.maximum(late_ref[...], best[0:1, :])
        early_ref[...] = jnp.maximum(early_ref[...], best[1:2, :])

    with jax.named_scope("rowin"):
        send(row_out, row_in, row_send, row_sem, peer(1)).wait_recv()
        for h in range(1, 8):
            take(row_in.at[h - 1])
    with jax.named_scope("back"):
        back_copy(0).wait_recv()
        take(back_in.at[0])

        @if_two
        def _():
            @pl.when(x == 1)
            def _():
                send(two_in, two_in, twob_send, twob_recv, far_up).wait_recv()
                for k in range(2):
                    at = slice(k * unit, (k + 1) * unit)
                    early_ref[:, at] = jnp.maximum(early_ref[:, at], two_in[k, 0:1, :])

        if wrap:
            @pl.when(last == 1)
            def _():
                back_copy(1).wait_recv()
                take(back_in.at[1])

    with jax.named_scope("drain"):
        core_copy(every).wait_send()
        x_copy(0, every).wait_send()
        y_copy(0, every).wait_send()
        z_copy(0, every).wait_send()
        diag_copy(0, True, every).wait_send()
        for k in range(3):
            twin_copy(k, 0, every).wait_send()

        @if_two
        def _():
            two_copy(0, unit).wait_send()
            twob_copy(0).wait_send()

        send(row_out, row_in, row_send, row_sem, peer(1)).wait_send()
        back_copy(0).wait_send()

        @if_relay
        def _():
            relay_copy(0, every).wait_send()
            back_copy(1).wait_send()


def kernel(blocks, copies, *refs):
    dma = pltpu.SemaphoreType.DMA
    pl.run_scoped(
        functools.partial(program, blocks, copies, *refs),
        dma((CHUNKS,)), dma,
        dma, dma, dma, dma((CHUNKS,)), dma, dma((CHUNKS,)), dma, dma((2,)), dma((2 * CHUNKS,)),
        dma, dma, dma((CHUNKS,)), dma((3,)), dma((3, 2)), dma, dma,
        dma, dma, dma((2,)), dma((2,)), dma, dma,
    )


def shards(embeddings, ranks):
    rows, width = embeddings.shape
    copies = lax.axis_size("rep")
    blocks = lax.axis_size("blk")
    lines = rows // LANES
    vmem = pl.BlockSpec(memory_space=pltpu.VMEM)
    hbm = pl.BlockSpec(memory_space=pltpu.HBM)
    f32, i32, bf16 = jnp.float32, jnp.int32, jnp.bfloat16
    both = pl.pallas_call(
        functools.partial(kernel, blocks, copies),
        out_shape=jax.ShapeDtypeStruct((2, rows), f32),
        in_specs=[hbm, hbm],
        out_specs=vmem,
        scratch_shapes=[
            pltpu.VMEM((rows, width), f32),
            pltpu.VMEM((3, 2 * copies * lines, LANES), i32),
            pltpu.VMEM((9, rows, width), bf16),
            pltpu.VMEM((rows, width), bf16),
            pltpu.VMEM((rows // 2, width), bf16),
            pltpu.VMEM((2, rows, LANES), i32),
            pltpu.VMEM((rows, LANES), i32),
            pltpu.VMEM((rows // 2, LANES), i32),
            pltpu.VMEM((2, rows, LANES), f32),
            pltpu.VMEM((rows, LANES), f32),
            pltpu.VMEM((rows // 2, LANES), f32),
            pltpu.VMEM((8, 8, rows), f32),
            pltpu.VMEM((4, 8, rows), f32),
            pltpu.VMEM((7, 2, rows), f32),
            pltpu.VMEM((7, 2, rows), f32),
            pltpu.VMEM((2, 2, rows), f32),
            pltpu.VMEM((2, 2, rows), f32),
            pltpu.VMEM((2, rows // 2), f32),
            pltpu.VMEM((2, 2, rows // 2), f32),
        ],
        compiler_params=pltpu.CompilerParams(
            collective_id=0, has_side_effects=True, vmem_limit_bytes=56_500_000
        ),
    )(embeddings, ranks.reshape(-1, LANES))
    return both[0], both[1]


def solution(mesh):
    return jax.shard_map(
        shards,
        mesh=mesh,
        in_specs=(P(("blk", "rep"), None), P()),
        out_specs=(P(("blk", "rep")), P(("blk", "rep"))),
        check_vma=False,
    )
```

```python
import functools

import jax
import jax.numpy as jnp
from jax import lax
from jax.experimental import pallas as pl
from jax.experimental.pallas import tpu as pltpu
from jax.sharding import PartitionSpec as P

CHUNKS = 8
LANES = 128
MESH = pl.DeviceIdType.MESH


def program(
    blocks, copies, emb_hbm, ranks_hbm, out_ref,
    emb, rank, mem, pair, two,
    guest_rank, pair_rank, two_rank, guest_acc, pair_acc, two_acc, host_acc, swap_acc,
    row_out, row_in, back_out, back_in, two_out, two_in,
    emb_sem, rank_sem,
    core_send, core_recv, x_send, x_recv, y_send, y_recv, z_send, z_recv, pair_recv,
    relay_send, diag_send, diag_recv, twin_send, twin_recv, two_send, two_recv,
    row_send, row_sem, back_send, back_recv, twob_send, twob_recv, drained,
):
    rows = emb.shape[0]
    early_ref, late_ref = out_ref.at[0:1], out_ref.at[1:2]
    part = rows // CHUNKS
    unit = rows // 2
    small = part // 2
    half = CHUNKS // 2
    lines = rows // LANES
    layers = blocks // 2
    wrap = layers == 4

    b = blocks - 1 - lax.axis_index("blk")
    r = lax.axis_index("rep")
    x = lax.rem(b, 2)
    l = b // 2

    def flip_rep(k):
        dy, dc = k // 2, k % 2
        y, c = r // 2, lax.rem(r, 2)
        return 2 * (y + dy - 2 * y * dy) + c + dc - 2 * c * dc

    def flip_x(d):
        return x + d - 2 * x * d

    def device(row, column, copy):
        return (blocks - 1 - 2 * row - column, copy)

    def peer(h):
        return device(l, flip_x(h // 4), flip_rep(h % 4))

    def layer(offset):
        return lax.rem(l + offset + layers, layers)

    if wrap:
        last = l // (layers - 1)
        is_relay = l == 1
        has_two = lax.rem(l, 2) == 0
        two_turn = l // 2
    else:
        last = 0 * l
        is_relay = None
        has_two = None
        two_turn = 0 * l

    def if_relay(f):
        if wrap:
            pl.when(is_relay)(f)

    def unless_relay(f):
        if wrap:
            pl.when(l != 1)(f)
        else:
            f()

    def if_two(f):
        if wrap:
            pl.when(has_two)(f)
        else:
            f()

    up = device(layer(1), x, r)
    down = device(layer(-1), x, r)
    cross = flip_rep(1)
    far_up = device(layer(2), x, r)
    far_down = device(layer(-2), x, r)
    cross_up = device(layer(2), x, cross)
    cross_down = device(layer(-2), x, cross)
    relay_to = device(layer(-1), x, cross)

    def cut(i):
        return pl.ds(pl.multiple_of(i * part, part), part)

    def emb_copy(i):
        return pltpu.make_async_copy(emb_hbm.at[cut(i)], emb.at[cut(i)], emb_sem.at[i])

    def rank_copy(k):
        size = 2 * copies * lines
        return pltpu.make_async_copy(
            ranks_hbm.at[pl.ds(pl.multiple_of((layers - 1 - layer(-k)) * size, size), size)],
            rank.at[k], rank_sem,
        )

    barrier = pltpu.get_barrier_semaphore()

    def greet(target):
        pl.semaphore_signal(barrier, inc=1, device_id=target, device_id_type=MESH)

    for h in (1, 2, 4):
        greet(peer(h))
    if wrap:
        @pl.when(l == 0)
        def _():
            greet(device(l + 1, x, cross))

        @pl.when(l > 0)
        def _():
            greet(down)

        @pl.when(is_relay)
        def _():
            greet(cross_up)

        @pl.when(has_two)
        def _():
            greet(far_up)

        expected = 5 - last
    else:
        greet(down)
        greet(far_down)
        expected = 5

    for i in range(CHUNKS):
        emb_copy(i).start()
    for k in range(3):
        rank_copy(k).start()

    def send(src, dst, send_sem, recv_sem, device):
        return pltpu.make_async_remote_copy(
            src_ref=src, dst_ref=dst, send_sem=send_sem, recv_sem=recv_sem,
            device_id=device, device_id_type=MESH,
        )

    def host(h):
        return mem.at[h + 1]

    def area(u):
        return pl.ds(pl.multiple_of(u * unit, unit), unit)

    every = pl.ds(0, rows)

    def core_copy(at):
        return send(host(0).at[at], host(1).at[at], core_send, core_recv, peer(1))

    def x_copy(i, at=None):
        at = cut(i) if at is None else at
        return send(host(0).at[at], host(4).at[at], x_send, x_recv.at[i], peer(4))

    def y_copy(i, at=None):
        at = cut(i) if at is None else at
        return send(host(0).at[at], host(2).at[at], y_send, y_recv.at[i], peer(2))

    def z_copy(u, at):
        return send(host(0).at[at], mem.at[0, at], z_send, z_recv.at[u], up)

    def far_copy(k, at):
        return send(host(0).at[at], pair.at[at], z_send, pair_recv.at[k], cross_down)

    def relay_copy(u, at):
        return send(pair.at[at], mem.at[0, at], relay_send, z_recv.at[u], relay_to)

    def diag_copy(i, by_x, at=None):
        at = cut(i) if at is None else at
        source, target = (2, peer(4)) if by_x else (4, peer(2))
        return send(host(source).at[at], host(6).at[at], diag_send, diag_recv.at[i], target)

    def twin_copy(k, u, at):
        slot = 2 + 2 * k
        return send(
            host(slot).at[at], host(slot + 1).at[at], twin_send.at[k], twin_recv.at[k, u], peer(1)
        )

    def two_copy(i, size):
        at = pl.ds(pl.multiple_of(x * unit + i * part, part), size)
        there = pl.ds(i * part, size)
        return send(host(4 * (1 - x)).at[at], two.at[there], two_send, two_recv, far_up)

    def normalise(i):
        emb_copy(i).wait()
        v = emb[cut(i), :]
        squares = jnp.sum(v * v, axis=1, keepdims=True)
        mem[1, cut(i), :] = (v * lax.rsqrt(squares + 1e-06)).astype(jnp.bfloat16)

    def piece(k):
        return pl.ds(pl.multiple_of(k * small, small), small)

    def ascend(i):
        def far():
            for n in range(part // small):
                k = i * (part // small) + n
                far_copy(k, piece(k)).start()

        if wrap:
            pl.when(last == 1)(far)

            @pl.when(last == 0)
            def _():
                z_copy(i // half, cut(i)).start()
        else:
            z_copy(i // half, cut(i)).start()

    def launch(i):
        ascend(i)
        x_copy(i).start()
        y_copy(i).start()
        core_copy(cut(i)).start()

    with jax.named_scope("norm"):
        normalise(0)
        normalise(1)
    with jax.named_scope("barrier"):
        pl.semaphore_wait(barrier, expected)

    def prepare(i, _):
        launch(i - 2)
        normalise(i)
        return 0

    with jax.named_scope("prepare"):
        launch(0)
        normalise(2)
        lax.fori_loop(3, CHUNKS, prepare, 0)
        for k in range(3):
            rank_copy(k).wait()
        launch(CHUNKS - 2)
        launch(CHUNKS - 1)

    def relay(i):
        for n in range(part // small):
            k = i * (part // small) + n
            with jax.named_scope("w"):
                far_copy(k, piece(k)).wait_recv()
            relay_copy(i // half, piece(k)).start()

        @pl.when(i == CHUNKS - 1)
        def _():
            pl.semaphore_signal(drained, inc=1, device_id=up, device_id_type=MESH)

    sign = 2 * x - 1

    def place(column, copy):
        return (copies * (1 - column) + copy) * lines

    def spread(slot, row, count, out, factor=None):
        for g in range(count):
            line = rank[slot, pl.ds(row + g, 1), :]
            if factor is not None:
                line = line * factor
            out[g * LANES:(g + 1) * LANES, :] = jnp.broadcast_to(line, (LANES, LANES)).T

    spread(0, place(x, r), lines, guest_rank.at[1])
    for acc in (guest_acc, pair_acc, two_acc, host_acc, swap_acc):
        acc[...] = jnp.full(acc.shape, -1.0, jnp.float32)

    def score(guest, guest_line, best_ref, h, u, acc, slot, factor=None, slots=1):
        if u is None:
            low, size = 0, rows
            hosts = mem[pl.ds(h + 1, slots)].reshape(slots * rows, mem.shape[2])
        else:
            low, size = u * unit, unit
            hosts = mem[h + 1, area(u), :]
        count = guest_line.size // LANES
        lhs = guest[...].reshape(count, hosts.shape[1])
        scores = lax.dot_general(
            lhs, hosts, (((1,), (1,)), ((), ())), preferred_element_type=jnp.float32
        )
        own = guest_line[...].reshape(count, LANES)
        best = best_ref[...].reshape(count, LANES)
        for k in range(slots):
            row = place(flip_x((h + k) // 4), flip_rep((h + k) % 4))
            for g in range(size // LANES):
                line = rank[0, pl.ds(row + low // LANES + g, 1), :]
                if factor is not None:
                    line = line * factor
                at = slice(k * size + g * LANES, k * size + (g + 1) * LANES)
                kept = jnp.where(line < own, scores[:, at], jnp.float32(-1.0))
                best = jnp.maximum(best, kept)
                column = jnp.max(kept.reshape(count // 8, 8, LANES), axis=0)
                there = pl.ds(pl.multiple_of(low + g * LANES, LANES), LANES)
                acc[slot + k, :, there] = jnp.maximum(acc[slot + k, :, there], column)
        best_ref[...] = best.reshape(best_ref.shape)

    def own_score(h, u=None):
        score(mem.at[1], guest_rank.at[1], guest_acc.at[1], h, u, host_acc, h)

    def up_score(h, u=None):
        score(mem.at[0], guest_rank.at[0], guest_acc.at[0], h, u, host_acc, h)

    def both_score(h, u):
        score(mem.at[0:2], guest_rank, guest_acc, h, u, host_acc, h)

    def part_score(v, h, u=None):
        at = slice(v * unit, (v + 1) * unit)
        score(mem.at[0, at], guest_rank.at[0, at], guest_acc.at[0, at], h, u, host_acc, h)

    def pair_score(h):
        score(pair, pair_rank, pair_acc, h, None, swap_acc, h - 4, sign, slots=2)

    def two_score(h):
        score(two, two_rank, two_acc, h, None, host_acc, h, slots=4)

    def sweep(f, low, high):
        def body(h, _):
            f(h)
            return 0
        lax.fori_loop(low, high, body, 0)

    def each(f, low, high):
        def body(i, _):
            f(i)
            return 0
        lax.fori_loop(low, high, body, 0)

    with jax.named_scope("own0"):
        own_score(0)
    spread(1, place(x, r), lines, guest_rank.at[0])
    spread(2, place(x, cross), lines, pair_rank, sign)
    spread(2, place(1, r) + x * (lines // 2), lines // 2, two_rank)
    with jax.named_scope("core"):
        core_copy(every).wait_recv()
    with jax.named_scope("own1"):
        own_score(1)

    def arrive(p, u):
        for by_x in (True, False):
            i = 2 * p + (0 if by_x else 1)

            @if_relay
            def _():
                relay(i)
                if u == 1:
                    k = i - half

                    @pl.when(k < 4 - 2 * x)
                    def _():
                        own_score(2 + k, 0)

                    @pl.when(k < 2)
                    def _():
                        part_score(0, k)

            with jax.named_scope("y"):
                y_copy(i).wait_recv()
            twin_copy(0, u, cut(i)).start()
            with jax.named_scope("x"):
                x_copy(i).wait_recv()
            twin_copy(1, u, cut(i)).start()
            diag_copy(i, by_x).start()

    def two_post(u):
        @if_two
        def _():
            @pl.when(two_turn == u)
            def _():
                two_copy(0, unit).start()

    def z_wait(u):
        with jax.named_scope("z"):
            z_copy(u, area(u)).wait_recv()

    for u in range(2):
        each(lambda p: arrive(p, u), u * (half // 2), (u + 1) * (half // 2))
        with jax.named_scope("twin"):
            for k in range(2):
                twin_copy(k, u, area(u)).wait_recv()

        if u == 0:
            two_post(0)

            @unless_relay
            def _():
                with jax.named_scope("own25"):
                    sweep(lambda h: own_score(h, 0), 2, 6 - 2 * x)
                z_wait(0)
                with jax.named_scope("v0"):
                    sweep(lambda h: part_score(0, h), 0, 2)

            @if_relay
            def _():
                z_wait(0)

    def diag_arrive(i):
        diag_copy(i, True).wait_recv()
        twin_copy(2, i // half, cut(i)).start()

    def wait_drained():
        @if_two
        def _():
            @pl.when(two_turn == 1)
            def _():
                with jax.named_scope("drained"):
                    pl.semaphore_wait(drained, 1)

    def diag_pair(low):
        with jax.named_scope("diag"):
            each(diag_arrive, low, low + 2)

    def steady():
        if wrap:
            wait_drained()
        z_wait(1)
        with jax.named_scope("both"):
            sweep(lambda h: both_score(h, 1), 2, 2)
            two_post(1)
            sweep(lambda h: both_score(h, 1), 2, 6 - 2 * x)
            sweep(lambda h: up_score(h, 1), 6 - 2 * x, 6)
        diag_pair(0)
        with jax.named_scope("up"):
            sweep(lambda h: up_score(h, 0), 2, 6)
        diag_pair(2)
        with jax.named_scope("v1"):
            sweep(lambda h: part_score(1, h), 0, 2)

    def delayed():
        with jax.named_scope("own25"):
            sweep(lambda h: own_score(h, 1), 2, 6 - 2 * x)
        with jax.named_scope("v0"):
            sweep(lambda h: part_score(0, h), 2, 6)
        diag_pair(0)
        z_wait(1)

        def later(h):
            @pl.when(h == 2)
            def _():
                diag_pair(2)
            part_score(1, h)

        with jax.named_scope("v1"):
            sweep(later, 0, 6)

    if wrap:
        pl.when(l > 0)(steady)
        pl.when(l == 0)(delayed)
    else:
        steady()
    diag_pair(half)

    def lanes(acc):
        return jnp.max(acc[...].T, axis=0, keepdims=True)

    none = jnp.full((1, rows), -1.0, jnp.float32)

    def back_copy(slot):
        target = cross_up if slot else device(layer(-1), x, r)
        return send(back_out.at[slot], back_in.at[slot], back_send.at[slot], back_recv.at[slot], target)

    def last_score(t):
        u, odd = t // 2, lax.rem(t, 2)

        @pl.when(t == 2)
        def _():
            diag_pair(half + 2)

        @pl.when(odd == 1)
        def _():
            with jax.named_scope("twin2"):
                twin_copy(2, u, area(u)).wait_recv()

        @pl.when(x == 0)
        def _():
            both_score(6 + odd, u)

        @pl.when(x == 1)
        def _():
            up_score(6 + odd, u)

        @if_relay
        def _():
            @pl.when(odd == u)
            def _():
                with jax.named_scope("pair"):
                    pair_score(4 + t - odd)

    with jax.named_scope("last"):
        each(last_score, 0, 4)

    @if_relay
    def _():
        best = lanes(pair_acc)
        back_out[1, 0:1, :] = jnp.where(x == 0, best, none)
        back_out[1, 1:2, :] = jnp.where(x == 0, none, best)
        back_copy(1).start()

    back_out[0, 0:1, :] = none
    back_out[0, 1:2, :] = lanes(guest_acc.at[0])
    back_copy(0).start()

    def twob_copy(k):
        return send(two_out, two_in.at[k], twob_send, twob_recv, device(layer(-2), 1, r))

    def row_copy(h):
        return send(row_out.at[h - 1], row_in.at[h - 1], row_send, row_sem, peer(h))

    def row_post(h):
        row_out[h - 1, 0:1, :] = jnp.max(host_acc[h], axis=0, keepdims=True)
        row_out[h - 1, 1:2, :] = none
        row_copy(h).start()

    @unless_relay
    def _():
        sweep(row_post, 4 - 3 * x, 8 - 4 * x)

    def row_merge(h):
        best = jnp.max(host_acc[h], axis=0, keepdims=True)
        swapped = jnp.max(swap_acc[h - 4], axis=0, keepdims=True)
        row_out[h - 1, 0:1, :] = jnp.where(x == 0, best, jnp.maximum(best, swapped))
        row_out[h - 1, 1:2, :] = jnp.where(x == 0, swapped, none)
        row_copy(h).start()

    @if_relay
    def _():
        sweep(row_merge, 4, 8)
        sweep(row_post, 1, 4)

    @if_two
    def _():
        with jax.named_scope("two"):
            two_copy(0, unit).wait_recv()
        with jax.named_scope("v2"):
            two_score(4 * x)
        two_out[...] = jnp.broadcast_to(lanes(two_acc), two_out.shape)
        twob_copy(x).start()

    with jax.named_scope("rows"):
        @unless_relay
        def _():
            sweep(row_post, 1 + 3 * x, 4 + 4 * x)

    late_ref[...] = jnp.max(host_acc[0], axis=0, keepdims=True)
    early_ref[...] = lanes(guest_acc.at[1])

    def take(best):
        late_ref[...] = jnp.maximum(late_ref[...], best[0:1, :])
        early_ref[...] = jnp.maximum(early_ref[...], best[1:2, :])

    with jax.named_scope("rowin"):
        send(row_out, row_in, row_send, row_sem, peer(1)).wait_recv()
        for h in range(1, 8):
            take(row_in.at[h - 1])
    with jax.named_scope("back"):
        back_copy(0).wait_recv()
        take(back_in.at[0])

        @if_two
        def _():
            @pl.when(x == 1)
            def _():
                send(two_in, two_in, twob_send, twob_recv, far_up).wait_recv()
                for k in range(2):
                    at = slice(k * unit, (k + 1) * unit)
                    early_ref[:, at] = jnp.maximum(early_ref[:, at], two_in[k, 0:1, :])

        if wrap:
            @pl.when(last == 1)
            def _():
                back_copy(1).wait_recv()
                take(back_in.at[1])

    with jax.named_scope("drain"):
        core_copy(every).wait_send()
        x_copy(0, every).wait_send()
        y_copy(0, every).wait_send()
        z_copy(0, every).wait_send()
        diag_copy(0, True, every).wait_send()
        for k in range(3):
            twin_copy(k, 0, every).wait_send()

        @if_two
        def _():
            two_copy(0, unit).wait_send()
            twob_copy(0).wait_send()

        send(row_out, row_in, row_send, row_sem, peer(1)).wait_send()
        back_copy(0).wait_send()

        @if_relay
        def _():
            relay_copy(0, every).wait_send()
            back_copy(1).wait_send()


def kernel(blocks, copies, *refs):
    dma = pltpu.SemaphoreType.DMA
    pl.run_scoped(
        functools.partial(program, blocks, copies, *refs),
        dma((CHUNKS,)), dma,
        dma, dma, dma, dma((CHUNKS,)), dma, dma((CHUNKS,)), dma, dma((2,)), dma((2 * CHUNKS,)),
        dma, dma, dma((CHUNKS,)), dma((3,)), dma((3, 2)), dma, dma,
        dma, dma, dma((2,)), dma((2,)), dma, dma, pltpu.SemaphoreType.REGULAR,
    )


def shards(embeddings, ranks):
    rows, width = embeddings.shape
    copies = lax.axis_size("rep")
    blocks = lax.axis_size("blk")
    lines = rows // LANES
    vmem = pl.BlockSpec(memory_space=pltpu.VMEM)
    hbm = pl.BlockSpec(memory_space=pltpu.HBM)
    f32, i32, bf16 = jnp.float32, jnp.int32, jnp.bfloat16
    both = pl.pallas_call(
        functools.partial(kernel, blocks, copies),
        out_shape=jax.ShapeDtypeStruct((2, rows), f32),
        in_specs=[hbm, hbm],
        out_specs=vmem,
        scratch_shapes=[
            pltpu.VMEM((rows, width), f32),
            pltpu.VMEM((3, 2 * copies * lines, LANES), i32),
            pltpu.VMEM((9, rows, width), bf16),
            pltpu.VMEM((rows, width), bf16),
            pltpu.VMEM((rows // 2, width), bf16),
            pltpu.VMEM((2, rows, LANES), i32),
            pltpu.VMEM((rows, LANES), i32),
            pltpu.VMEM((rows // 2, LANES), i32),
            pltpu.VMEM((2, rows, LANES), f32),
            pltpu.VMEM((rows, LANES), f32),
            pltpu.VMEM((rows // 2, LANES), f32),
            pltpu.VMEM((8, 8, rows), f32),
            pltpu.VMEM((4, 8, rows), f32),
            pltpu.VMEM((7, 2, rows), f32),
            pltpu.VMEM((7, 2, rows), f32),
            pltpu.VMEM((2, 2, rows), f32),
            pltpu.VMEM((2, 2, rows), f32),
            pltpu.VMEM((2, rows // 2), f32),
            pltpu.VMEM((2, 2, rows // 2), f32),
        ],
        compiler_params=pltpu.CompilerParams(
            collective_id=0, has_side_effects=True, vmem_limit_bytes=56_500_000
        ),
    )(embeddings, ranks.reshape(-1, LANES))
    return both[0], both[1]


def solution(mesh):
    return jax.shard_map(
        shards,
        mesh=mesh,
        in_specs=(P(("blk", "rep"), None), P()),
        out_specs=(P(("blk", "rep")), P(("blk", "rep"))),
        check_vma=False,
    )
```

```python
import functools

import jax
import jax.numpy as jnp
from jax import lax
from jax.experimental import pallas as pl
from jax.experimental.pallas import tpu as pltpu
from jax.sharding import PartitionSpec as P

CHUNKS = 8
LANES = 128
MESH = pl.DeviceIdType.MESH


def program(
    blocks, copies, emb_hbm, ranks_hbm, out_ref,
    emb, rank, mem, pair, two,
    guest_rank, pair_rank, two_rank, guest_acc, pair_acc, two_acc, host_acc, swap_acc,
    row_out, row_in, back_out, back_in, two_out, two_in,
    emb_sem, rank_sem,
    core_send, core_recv, x_send, x_recv, y_send, y_recv, z_send, z_recv, pair_recv,
    relay_send, diag_send, diag_recv, twin_send, twin_recv, two_send, two_recv,
    row_send, row_sem, back_send, back_recv, twob_send, twob_recv, drained,
):
    rows = emb.shape[0]
    early_ref, late_ref = out_ref.at[0:1], out_ref.at[1:2]
    part = rows // CHUNKS
    unit = rows // 2
    small = part // 2
    head = part + small
    half = CHUNKS // 2
    lines = rows // LANES
    layers = blocks // 2
    wrap = layers == 4

    b = blocks - 1 - lax.axis_index("blk")
    r = lax.axis_index("rep")
    x = lax.rem(b, 2)
    l = b // 2

    def flip_rep(k):
        dy, dc = k // 2, k % 2
        y, c = r // 2, lax.rem(r, 2)
        return 2 * (y + dy - 2 * y * dy) + c + dc - 2 * c * dc

    def flip_x(d):
        return x + d - 2 * x * d

    def device(row, column, copy):
        return (blocks - 1 - 2 * row - column, copy)

    def peer(h):
        return device(l, flip_x(h // 4), flip_rep(h % 4))

    def layer(offset):
        return lax.rem(l + offset + layers, layers)

    if wrap:
        last = l // (layers - 1)
        is_relay = l == 1
        has_two = lax.rem(l, 2) == 0
        two_turn = l // 2
    else:
        last = 0 * l
        is_relay = None
        has_two = None
        two_turn = 0 * l

    def if_relay(f):
        if wrap:
            pl.when(is_relay)(f)

    def unless_relay(f):
        if wrap:
            pl.when(l != 1)(f)
        else:
            f()

    def if_two(f):
        if wrap:
            pl.when(has_two)(f)
        else:
            f()

    up = device(layer(1), x, r)
    down = device(layer(-1), x, r)
    cross = flip_rep(1)
    far_up = device(layer(2), x, r)
    far_down = device(layer(-2), x, r)
    cross_up = device(layer(2), x, cross)
    cross_down = device(layer(-2), x, cross)
    relay_to = device(layer(-1), x, cross)

    def cut(i):
        return pl.ds(pl.multiple_of(i * part, part), part)

    def emb_copy(i):
        return pltpu.make_async_copy(emb_hbm.at[cut(i)], emb.at[cut(i)], emb_sem.at[i])

    def rank_copy(k):
        size = 2 * copies * lines
        return pltpu.make_async_copy(
            ranks_hbm.at[pl.ds(pl.multiple_of((layers - 1 - layer(-k)) * size, size), size)],
            rank.at[k], rank_sem,
        )

    barrier = pltpu.get_barrier_semaphore()

    def greet(target):
        pl.semaphore_signal(barrier, inc=1, device_id=target, device_id_type=MESH)

    for h in (1, 2, 4):
        greet(peer(h))
    if wrap:
        @pl.when(l == 0)
        def _():
            greet(device(l + 1, x, cross))

        @pl.when(l > 0)
        def _():
            greet(down)

        @pl.when(is_relay)
        def _():
            greet(cross_up)

        @pl.when(has_two)
        def _():
            greet(far_up)

        expected = 5 - last
    else:
        greet(down)
        greet(far_down)
        expected = 5

    for i in range(CHUNKS):
        emb_copy(i).start()
    for k in range(3):
        rank_copy(k).start()

    def send(src, dst, send_sem, recv_sem, device):
        return pltpu.make_async_remote_copy(
            src_ref=src, dst_ref=dst, send_sem=send_sem, recv_sem=recv_sem,
            device_id=device, device_id_type=MESH,
        )

    def host(h):
        return mem.at[h + 1]

    def area(u):
        return pl.ds(pl.multiple_of(u * unit, unit), unit)

    every = pl.ds(0, rows)

    def core_copy(at):
        return send(host(0).at[at], host(1).at[at], core_send, core_recv, peer(1))

    def x_copy(i, at=None):
        at = cut(i) if at is None else at
        return send(host(0).at[at], host(4).at[at], x_send, x_recv.at[i], peer(4))

    def y_copy(i, at=None):
        at = cut(i) if at is None else at
        return send(host(0).at[at], host(2).at[at], y_send, y_recv.at[i], peer(2))

    def z_copy(u, at):
        return send(host(0).at[at], mem.at[0, at], z_send, z_recv.at[u], up)

    def far_copy(k, at):
        return send(host(0).at[at], pair.at[at], z_send, pair_recv.at[k], cross_down)

    def relay_copy(u, at):
        return send(pair.at[at], mem.at[0, at], relay_send, z_recv.at[u], relay_to)

    def diag_copy(i, by_x, at=None):
        at = cut(i) if at is None else at
        source, target = (2, peer(4)) if by_x else (4, peer(2))
        return send(host(source).at[at], host(6).at[at], diag_send, diag_recv.at[i], target)

    def twin_copy(k, u, at):
        slot = 2 + 2 * k
        return send(
            host(slot).at[at], host(slot + 1).at[at], twin_send.at[k], twin_recv.at[k, u], peer(1)
        )

    def two_copy(i, size):
        at = pl.ds(pl.multiple_of(x * unit + i, small), size)
        there = pl.ds(i, size)
        return send(host(4 * (1 - x)).at[at], two.at[there], two_send, two_recv, far_up)

    def normalise(i):
        emb_copy(i).wait()
        v = emb[cut(i), :]
        squares = jnp.sum(v * v, axis=1, keepdims=True)
        mem[1, cut(i), :] = (v * lax.rsqrt(squares + 1e-06)).astype(jnp.bfloat16)

    def piece(k):
        return pl.ds(pl.multiple_of(k * small, small), small)

    def ascend(i):
        def far():
            for n in range(part // small):
                k = i * (part // small) + n
                far_copy(k, piece(k)).start()

        if wrap:
            pl.when(last == 1)(far)

            @pl.when(last == 0)
            def _():
                z_copy(i // half, cut(i)).start()
        else:
            z_copy(i // half, cut(i)).start()

    def launch(i):
        ascend(i)
        x_copy(i).start()
        y_copy(i).start()
        core_copy(cut(i)).start()

    with jax.named_scope("norm"):
        normalise(0)
        normalise(1)
    with jax.named_scope("barrier"):
        pl.semaphore_wait(barrier, expected)

    def prepare(i, _):
        launch(i - 2)
        normalise(i)
        return 0

    with jax.named_scope("prepare"):
        launch(0)
        normalise(2)
        lax.fori_loop(3, CHUNKS, prepare, 0)
        for k in range(3):
            rank_copy(k).wait()
        launch(CHUNKS - 2)
        launch(CHUNKS - 1)

    def relay(i):
        for n in range(part // small):
            k = i * (part // small) + n
            with jax.named_scope("w"):
                far_copy(k, piece(k)).wait_recv()
            relay_copy(i // half, piece(k)).start()


    sign = 2 * x - 1

    def place(column, copy):
        return (copies * (1 - column) + copy) * lines

    def spread(slot, row, count, out, factor=None):
        for g in range(count):
            line = rank[slot, pl.ds(row + g, 1), :]
            if factor is not None:
                line = line * factor
            out[g * LANES:(g + 1) * LANES, :] = jnp.broadcast_to(line, (LANES, LANES)).T

    spread(0, place(x, r), lines, guest_rank.at[1])
    for acc in (guest_acc, pair_acc, two_acc, host_acc, swap_acc):
        acc[...] = jnp.full(acc.shape, -1.0, jnp.float32)

    def score(guest, guest_line, best_ref, h, u, acc, slot, factor=None, slots=1):
        if u is None:
            low, size = 0, rows
            hosts = mem[pl.ds(h + 1, slots)].reshape(slots * rows, mem.shape[2])
        else:
            low, size = u * unit, unit
            hosts = mem[h + 1, area(u), :]
        count = guest_line.size // LANES
        lhs = guest[...].reshape(count, hosts.shape[1])
        scores = lax.dot_general(
            lhs, hosts, (((1,), (1,)), ((), ())), preferred_element_type=jnp.float32
        )
        own = guest_line[...].reshape(count, LANES)
        best = best_ref[...].reshape(count, LANES)
        for k in range(slots):
            row = place(flip_x((h + k) // 4), flip_rep((h + k) % 4))
            for g in range(size // LANES):
                line = rank[0, pl.ds(row + low // LANES + g, 1), :]
                if factor is not None:
                    line = line * factor
                at = slice(k * size + g * LANES, k * size + (g + 1) * LANES)
                kept = jnp.where(line < own, scores[:, at], jnp.float32(-1.0))
                best = jnp.maximum(best, kept)
                column = jnp.max(kept.reshape(count // 8, 8, LANES), axis=0)
                there = pl.ds(pl.multiple_of(low + g * LANES, LANES), LANES)
                acc[slot + k, :, there] = jnp.maximum(acc[slot + k, :, there], column)
        best_ref[...] = best.reshape(best_ref.shape)

    def own_score(h, u=None):
        score(mem.at[1], guest_rank.at[1], guest_acc.at[1], h, u, host_acc, h)

    def up_score(h, u=None):
        score(mem.at[0], guest_rank.at[0], guest_acc.at[0], h, u, host_acc, h)

    def both_score(h, u):
        score(mem.at[0:2], guest_rank, guest_acc, h, u, host_acc, h)

    def part_score(v, h, u=None):
        at = slice(v * unit, (v + 1) * unit)
        score(mem.at[0, at], guest_rank.at[0, at], guest_acc.at[0, at], h, u, host_acc, h)

    def pair_score(h):
        score(pair, pair_rank, pair_acc, h, None, swap_acc, h - 4, sign, slots=2)

    def two_score(h):
        score(two, two_rank, two_acc, h, None, host_acc, h, slots=4)

    def sweep(f, low, high):
        def body(h, _):
            f(h)
            return 0
        lax.fori_loop(low, high, body, 0)

    def each(f, low, high):
        def body(i, _):
            f(i)
            return 0
        lax.fori_loop(low, high, body, 0)

    with jax.named_scope("own0"):
        own_score(0)
    spread(1, place(x, r), lines, guest_rank.at[0])
    spread(2, place(x, cross), lines, pair_rank, sign)
    spread(2, place(1, r) + x * (lines // 2), lines // 2, two_rank)
    with jax.named_scope("core"):
        core_copy(every).wait_recv()
    with jax.named_scope("own1"):
        own_score(1)

    def arrive(p, u):
        for by_x in (True, False):
            i = 2 * p + (0 if by_x else 1)

            @if_relay
            def _():
                relay(i)
                if u == 1:
                    k = i - half

                    @pl.when(k < 4 - 2 * x)
                    def _():
                        own_score(2 + k, 0)

                    @pl.when(k < 2)
                    def _():
                        part_score(0, k)

            with jax.named_scope("y"):
                y_copy(i).wait_recv()
            twin_copy(0, u, cut(i)).start()
            with jax.named_scope("x"):
                x_copy(i).wait_recv()
            twin_copy(1, u, cut(i)).start()
            diag_copy(i, by_x).start()

    def two_post(turn, low, size):
        @if_two
        def _():
            @pl.when(two_turn == turn)
            def _():
                two_copy(low, size).start()

    def z_wait(u):
        with jax.named_scope("z"):
            z_copy(u, area(u)).wait_recv()

    for u in range(2):
        each(lambda p: arrive(p, u), u * (half // 2), (u + 1) * (half // 2))
        with jax.named_scope("twin"):
            for k in range(2):
                twin_copy(k, u, area(u)).wait_recv()

        if u == 0:
            two_post(0, 0, unit)

            @unless_relay
            def _():
                with jax.named_scope("own25"):
                    sweep(lambda h: own_score(h, 0), 2, 6 - 2 * x)
                z_wait(0)
                with jax.named_scope("v0"):
                    sweep(lambda h: part_score(0, h), 0, 2)

            @if_relay
            def _():
                z_wait(0)

    def diag_arrive(i):
        diag_copy(i, True).wait_recv()
        twin_copy(2, i // half, cut(i)).start()

    def hand_over():
        @if_relay
        def _():
            with jax.named_scope("relayed"):
                relay_copy(0, every).wait_send()
            pl.semaphore_signal(drained, inc=1, device_id=up, device_id_type=MESH)

        @pl.when(l == 2)
        def _():
            with jax.named_scope("drained"):
                pl.semaphore_wait(drained, 1)
            two_copy(head, unit - head).start()

    def diag_pair(low):
        with jax.named_scope("diag"):
            each(diag_arrive, low, low + 2)

    def steady():
        z_wait(1)
        if wrap:
            two_post(1, 0, head)
        with jax.named_scope("both"):
            sweep(lambda h: both_score(h, 1), 2, 3)
            if wrap:
                hand_over()
            sweep(lambda h: both_score(h, 1), 3, 6 - 2 * x)
            sweep(lambda h: up_score(h, 1), 6 - 2 * x, 6)
        diag_pair(0)
        with jax.named_scope("up"):
            sweep(lambda h: up_score(h, 0), 2, 6)
        diag_pair(2)
        with jax.named_scope("v1"):
            sweep(lambda h: part_score(1, h), 0, 2)

    def delayed():
        with jax.named_scope("own25"):
            sweep(lambda h: own_score(h, 1), 2, 6 - 2 * x)
        with jax.named_scope("v0"):
            sweep(lambda h: part_score(0, h), 2, 6)
        diag_pair(0)
        z_wait(1)

        def later(h):
            @pl.when(h == 2)
            def _():
                diag_pair(2)
            part_score(1, h)

        with jax.named_scope("v1"):
            sweep(later, 0, 6)

    if wrap:
        pl.when(l > 0)(steady)
        pl.when(l == 0)(delayed)
    else:
        steady()
    diag_pair(half)

    def lanes(acc):
        return jnp.max(acc[...].T, axis=0, keepdims=True)

    none = jnp.full((1, rows), -1.0, jnp.float32)

    def back_copy(slot):
        target = cross_up if slot else device(layer(-1), x, r)
        return send(back_out.at[slot], back_in.at[slot], back_send.at[slot], back_recv.at[slot], target)

    def last_score(t):
        u, odd = t // 2, lax.rem(t, 2)

        @pl.when(t == 2)
        def _():
            diag_pair(half + 2)

        @pl.when(odd == 1)
        def _():
            with jax.named_scope("twin2"):
                twin_copy(2, u, area(u)).wait_recv()

        @pl.when(x == 0)
        def _():
            both_score(6 + odd, u)

        @pl.when(x == 1)
        def _():
            up_score(6 + odd, u)

        @if_relay
        def _():
            @pl.when(odd == u)
            def _():
                with jax.named_scope("pair"):
                    pair_score(4 + t - odd)

    with jax.named_scope("last"):
        each(last_score, 0, 4)

    @if_relay
    def _():
        best = lanes(pair_acc)
        back_out[1, 0:1, :] = jnp.where(x == 0, best, none)
        back_out[1, 1:2, :] = jnp.where(x == 0, none, best)
        back_copy(1).start()

    back_out[0, 0:1, :] = none
    back_out[0, 1:2, :] = lanes(guest_acc.at[0])
    back_copy(0).start()

    def twob_copy(k):
        return send(two_out, two_in.at[k], twob_send, twob_recv, device(layer(-2), 1, r))

    def row_copy(h):
        return send(row_out.at[h - 1], row_in.at[h - 1], row_send, row_sem, peer(h))

    def row_post(h):
        row_out[h - 1, 0:1, :] = jnp.max(host_acc[h], axis=0, keepdims=True)
        row_out[h - 1, 1:2, :] = none
        row_copy(h).start()

    @unless_relay
    def _():
        sweep(row_post, 4 - 3 * x, 8 - 4 * x)

    def row_merge(h):
        best = jnp.max(host_acc[h], axis=0, keepdims=True)
        swapped = jnp.max(swap_acc[h - 4], axis=0, keepdims=True)
        row_out[h - 1, 0:1, :] = jnp.where(x == 0, best, jnp.maximum(best, swapped))
        row_out[h - 1, 1:2, :] = jnp.where(x == 0, swapped, none)
        row_copy(h).start()

    @if_relay
    def _():
        sweep(row_merge, 4, 8)
        sweep(row_post, 1, 4)

    @if_two
    def _():
        with jax.named_scope("two"):
            two_copy(0, unit).wait_recv()
        with jax.named_scope("v2"):
            two_score(4 * x)
        two_out[...] = jnp.broadcast_to(lanes(two_acc), two_out.shape)
        twob_copy(x).start()

    with jax.named_scope("rows"):
        @unless_relay
        def _():
            sweep(row_post, 1 + 3 * x, 4 + 4 * x)

    late_ref[...] = jnp.max(host_acc[0], axis=0, keepdims=True)
    early_ref[...] = lanes(guest_acc.at[1])

    def take(best):
        late_ref[...] = jnp.maximum(late_ref[...], best[0:1, :])
        early_ref[...] = jnp.maximum(early_ref[...], best[1:2, :])

    with jax.named_scope("rowin"):
        send(row_out, row_in, row_send, row_sem, peer(1)).wait_recv()
        for h in range(1, 8):
            take(row_in.at[h - 1])
    with jax.named_scope("back"):
        back_copy(0).wait_recv()
        take(back_in.at[0])

        @if_two
        def _():
            @pl.when(x == 1)
            def _():
                send(two_in, two_in, twob_send, twob_recv, far_up).wait_recv()
                for k in range(2):
                    at = slice(k * unit, (k + 1) * unit)
                    early_ref[:, at] = jnp.maximum(early_ref[:, at], two_in[k, 0:1, :])

        if wrap:
            @pl.when(last == 1)
            def _():
                back_copy(1).wait_recv()
                take(back_in.at[1])

    with jax.named_scope("drain"):
        core_copy(every).wait_send()
        x_copy(0, every).wait_send()
        y_copy(0, every).wait_send()
        z_copy(0, every).wait_send()
        diag_copy(0, True, every).wait_send()
        for k in range(3):
            twin_copy(k, 0, every).wait_send()

        @if_two
        def _():
            two_copy(0, unit).wait_send()
            twob_copy(0).wait_send()

        send(row_out, row_in, row_send, row_sem, peer(1)).wait_send()
        back_copy(0).wait_send()

        @if_relay
        def _():
            back_copy(1).wait_send()


def kernel(blocks, copies, *refs):
    dma = pltpu.SemaphoreType.DMA
    pl.run_scoped(
        functools.partial(program, blocks, copies, *refs),
        dma((CHUNKS,)), dma,
        dma, dma, dma, dma((CHUNKS,)), dma, dma((CHUNKS,)), dma, dma((2,)), dma((2 * CHUNKS,)),
        dma, dma, dma((CHUNKS,)), dma((3,)), dma((3, 2)), dma, dma,
        dma, dma, dma((2,)), dma((2,)), dma, dma, pltpu.SemaphoreType.REGULAR,
    )


def shards(embeddings, ranks):
    rows, width = embeddings.shape
    copies = lax.axis_size("rep")
    blocks = lax.axis_size("blk")
    lines = rows // LANES
    vmem = pl.BlockSpec(memory_space=pltpu.VMEM)
    hbm = pl.BlockSpec(memory_space=pltpu.HBM)
    f32, i32, bf16 = jnp.float32, jnp.int32, jnp.bfloat16
    both = pl.pallas_call(
        functools.partial(kernel, blocks, copies),
        out_shape=jax.ShapeDtypeStruct((2, rows), f32),
        in_specs=[hbm, hbm],
        out_specs=vmem,
        scratch_shapes=[
            pltpu.VMEM((rows, width), f32),
            pltpu.VMEM((3, 2 * copies * lines, LANES), i32),
            pltpu.VMEM((9, rows, width), bf16),
            pltpu.VMEM((rows, width), bf16),
            pltpu.VMEM((rows // 2, width), bf16),
            pltpu.VMEM((2, rows, LANES), i32),
            pltpu.VMEM((rows, LANES), i32),
            pltpu.VMEM((rows // 2, LANES), i32),
            pltpu.VMEM((2, rows, LANES), f32),
            pltpu.VMEM((rows, LANES), f32),
            pltpu.VMEM((rows // 2, LANES), f32),
            pltpu.VMEM((8, 8, rows), f32),
            pltpu.VMEM((4, 8, rows), f32),
            pltpu.VMEM((7, 2, rows), f32),
            pltpu.VMEM((7, 2, rows), f32),
            pltpu.VMEM((2, 2, rows), f32),
            pltpu.VMEM((2, 2, rows), f32),
            pltpu.VMEM((2, rows // 2), f32),
            pltpu.VMEM((2, 2, rows // 2), f32),
        ],
        compiler_params=pltpu.CompilerParams(
            collective_id=0, has_side_effects=True, vmem_limit_bytes=56_500_000
        ),
    )(embeddings, ranks.reshape(-1, LANES))
    return both[0], both[1]


def solution(mesh):
    return jax.shard_map(
        shards,
        mesh=mesh,
        in_specs=(P(("blk", "rep"), None), P()),
        out_specs=(P(("blk", "rep")), P(("blk", "rep"))),
        check_vma=False,
    )
```

```python
import functools

import jax
import jax.numpy as jnp
from jax import lax
from jax.experimental import pallas as pl
from jax.experimental.pallas import tpu as pltpu
from jax.sharding import PartitionSpec as P

CHUNKS = 8
LANES = 128
MESH = pl.DeviceIdType.MESH


def program(
    blocks, copies, emb_hbm, ranks_hbm, out_ref,
    emb, rank, mem, pair, two,
    guest_rank, pair_rank, two_rank, guest_acc, pair_acc, two_acc, host_acc, swap_acc,
    row_out, row_in, back_out, back_in, two_out, two_in,
    emb_sem, rank_sem,
    core_send, core_recv, x_send, x_recv, y_send, y_recv, z_send, z_recv, pair_recv,
    relay_send, diag_send, diag_recv, twin_send, twin_recv, two_send, two_recv,
    row_send, row_sem, back_send, back_recv, twob_send, twob_recv, drained,
):
    rows = emb.shape[0]
    early_ref, late_ref = out_ref.at[0:1], out_ref.at[1:2]
    part = rows // CHUNKS
    unit = rows // 2
    small = part // 2
    head = part + small
    half = CHUNKS // 2
    lines = rows // LANES
    layers = blocks // 2
    wrap = layers == 4

    b = blocks - 1 - lax.axis_index("blk")
    r = lax.axis_index("rep")
    x = lax.rem(b, 2)
    l = b // 2

    def flip_rep(k):
        dy, dc = k // 2, k % 2
        y, c = r // 2, lax.rem(r, 2)
        return 2 * (y + dy - 2 * y * dy) + c + dc - 2 * c * dc

    def flip_x(d):
        return x + d - 2 * x * d

    def device(row, column, copy):
        return (blocks - 1 - 2 * row - column, copy)

    def peer(h):
        return device(l, flip_x(h // 4), flip_rep(h % 4))

    def layer(offset):
        return lax.rem(l + offset + layers, layers)

    if wrap:
        last = l // (layers - 1)
        is_relay = l == 1
        has_two = lax.rem(l, 2) == 0
        two_turn = l // 2
    else:
        last = 0 * l
        is_relay = None
        has_two = None
        two_turn = 0 * l

    def if_relay(f):
        if wrap:
            pl.when(is_relay)(f)

    def unless_relay(f):
        if wrap:
            pl.when(l != 1)(f)
        else:
            f()

    def if_two(f):
        if wrap:
            pl.when(has_two)(f)
        else:
            f()

    up = device(layer(1), x, r)
    down = device(layer(-1), x, r)
    cross = flip_rep(1)
    far_up = device(layer(2), x, r)
    far_down = device(layer(-2), x, r)
    cross_up = device(layer(2), x, cross)
    cross_down = device(layer(-2), x, cross)
    relay_to = device(layer(-1), x, cross)

    def cut(i):
        return pl.ds(pl.multiple_of(i * part, part), part)

    def emb_copy(i):
        return pltpu.make_async_copy(emb_hbm.at[cut(i)], emb.at[cut(i)], emb_sem.at[i])

    def rank_copy(k):
        size = 2 * copies * lines
        return pltpu.make_async_copy(
            ranks_hbm.at[pl.ds(pl.multiple_of((layers - 1 - layer(-k)) * size, size), size)],
            rank.at[k], rank_sem,
        )

    emb_copy(0).start()
    emb_copy(1).start()

    barrier = pltpu.get_barrier_semaphore()

    def greet(target):
        pl.semaphore_signal(barrier, inc=1, device_id=target, device_id_type=MESH)

    for h in (1, 2, 4):
        greet(peer(h))
    if wrap:
        @pl.when(l == 0)
        def _():
            greet(device(l + 1, x, cross))

        @pl.when(l > 0)
        def _():
            greet(down)

        @pl.when(is_relay)
        def _():
            greet(cross_up)

        @pl.when(has_two)
        def _():
            greet(far_up)

        expected = 5 - last
    else:
        greet(down)
        greet(far_down)
        expected = 5

    for i in range(2, CHUNKS):
        emb_copy(i).start()
    for k in range(3):
        rank_copy(k).start()

    def send(src, dst, send_sem, recv_sem, device):
        return pltpu.make_async_remote_copy(
            src_ref=src, dst_ref=dst, send_sem=send_sem, recv_sem=recv_sem,
            device_id=device, device_id_type=MESH,
        )

    def host(h):
        return mem.at[h + 1]

    def area(u):
        return pl.ds(pl.multiple_of(u * unit, unit), unit)

    every = pl.ds(0, rows)

    def core_copy(at):
        return send(host(0).at[at], host(1).at[at], core_send, core_recv, peer(1))

    def x_copy(i, at=None):
        at = cut(i) if at is None else at
        return send(host(0).at[at], host(4).at[at], x_send, x_recv.at[i], peer(4))

    def y_copy(i, at=None):
        at = cut(i) if at is None else at
        return send(host(0).at[at], host(2).at[at], y_send, y_recv.at[i], peer(2))

    def z_copy(u, at):
        return send(host(0).at[at], mem.at[0, at], z_send, z_recv.at[u], up)

    def far_copy(k, at):
        return send(host(0).at[at], pair.at[at], z_send, pair_recv.at[k], cross_down)

    def relay_copy(u, at):
        return send(pair.at[at], mem.at[0, at], relay_send, z_recv.at[u], relay_to)

    def diag_copy(i, by_x, at=None):
        at = cut(i) if at is None else at
        source, target = (2, peer(4)) if by_x else (4, peer(2))
        return send(host(source).at[at], host(6).at[at], diag_send, diag_recv.at[i], target)

    def twin_copy(k, u, at):
        slot = 2 + 2 * k
        return send(
            host(slot).at[at], host(slot + 1).at[at], twin_send.at[k], twin_recv.at[k, u], peer(1)
        )

    def two_copy(i, size):
        at = pl.ds(pl.multiple_of(x * unit + i, small), size)
        there = pl.ds(i, size)
        return send(host(4 * (1 - x)).at[at], two.at[there], two_send, two_recv, far_up)

    def normalise(i):
        emb_copy(i).wait()
        v = emb[cut(i), :]
        squares = jnp.sum(v * v, axis=1, keepdims=True)
        mem[1, cut(i), :] = (v * lax.rsqrt(squares + 1e-06)).astype(jnp.bfloat16)

    def piece(k):
        return pl.ds(pl.multiple_of(k * small, small), small)

    def ascend(i):
        def far():
            for n in range(part // small):
                k = i * (part // small) + n
                far_copy(k, piece(k)).start()

        if wrap:
            pl.when(last == 1)(far)

            @pl.when(last == 0)
            def _():
                z_copy(i // half, cut(i)).start()
        else:
            z_copy(i // half, cut(i)).start()

    def launch(i):
        ascend(i)
        x_copy(i).start()
        y_copy(i).start()
        core_copy(cut(i)).start()

    with jax.named_scope("norm"):
        normalise(0)
        normalise(1)
    with jax.named_scope("barrier"):
        pl.semaphore_wait(barrier, expected)

    def prepare(i, _):
        launch(i - 2)
        normalise(i)
        return 0

    with jax.named_scope("prepare"):
        launch(0)
        normalise(2)
        lax.fori_loop(3, CHUNKS, prepare, 0)
        for k in range(3):
            rank_copy(k).wait()
        launch(CHUNKS - 2)
        launch(CHUNKS - 1)

    def relay(i):
        for n in range(part // small):
            k = i * (part // small) + n
            with jax.named_scope("w"):
                far_copy(k, piece(k)).wait_recv()
            relay_copy(i // half, piece(k)).start()


    sign = 2 * x - 1

    def place(column, copy):
        return (copies * (1 - column) + copy) * lines

    def spread(slot, row, count, out, factor=None):
        for g in range(count):
            line = rank[slot, pl.ds(row + g, 1), :]
            if factor is not None:
                line = line * factor
            out[g * LANES:(g + 1) * LANES, :] = jnp.broadcast_to(line, (LANES, LANES)).T

    spread(0, place(x, r), lines, guest_rank.at[1])
    for acc in (guest_acc, pair_acc, two_acc, host_acc, swap_acc):
        acc[...] = jnp.full(acc.shape, -1.0, jnp.float32)

    def score(guest, guest_line, best_ref, h, u, acc, slot, factor=None, slots=1):
        if u is None:
            low, size = 0, rows
            hosts = mem[pl.ds(h + 1, slots)].reshape(slots * rows, mem.shape[2])
        else:
            low, size = u * unit, unit
            hosts = mem[h + 1, area(u), :]
        count = guest_line.size // LANES
        lhs = guest[...].reshape(count, hosts.shape[1])
        scores = lax.dot_general(
            lhs, hosts, (((1,), (1,)), ((), ())), preferred_element_type=jnp.float32
        )
        own = guest_line[...].reshape(count, LANES)
        best = best_ref[...].reshape(count, LANES)
        for k in range(slots):
            row = place(flip_x((h + k) // 4), flip_rep((h + k) % 4))
            for g in range(size // LANES):
                line = rank[0, pl.ds(row + low // LANES + g, 1), :]
                if factor is not None:
                    line = line * factor
                at = slice(k * size + g * LANES, k * size + (g + 1) * LANES)
                kept = jnp.where(line < own, scores[:, at], jnp.float32(-1.0))
                best = jnp.maximum(best, kept)
                column = jnp.max(kept.reshape(count // 8, 8, LANES), axis=0)
                there = pl.ds(pl.multiple_of(low + g * LANES, LANES), LANES)
                acc[slot + k, :, there] = jnp.maximum(acc[slot + k, :, there], column)
        best_ref[...] = best.reshape(best_ref.shape)

    def own_score(h, u=None):
        score(mem.at[1], guest_rank.at[1], guest_acc.at[1], h, u, host_acc, h)

    def up_score(h, u=None):
        score(mem.at[0], guest_rank.at[0], guest_acc.at[0], h, u, host_acc, h)

    def both_score(h, u):
        score(mem.at[0:2], guest_rank, guest_acc, h, u, host_acc, h)

    def part_score(v, h, u=None):
        at = slice(v * unit, (v + 1) * unit)
        score(mem.at[0, at], guest_rank.at[0, at], guest_acc.at[0, at], h, u, host_acc, h)

    def pair_score(h):
        score(pair, pair_rank, pair_acc, h, None, swap_acc, h - 4, sign, slots=2)

    def two_score(h):
        score(two, two_rank, two_acc, h, None, host_acc, h, slots=4)

    def sweep(f, low, high):
        def body(h, _):
            f(h)
            return 0
        lax.fori_loop(low, high, body, 0)

    def each(f, low, high):
        def body(i, _):
            f(i)
            return 0
        lax.fori_loop(low, high, body, 0)

    with jax.named_scope("own0"):
        own_score(0)
    spread(1, place(x, r), lines, guest_rank.at[0])
    spread(2, place(x, cross), lines, pair_rank, sign)
    spread(2, place(1, r) + x * (lines // 2), lines // 2, two_rank)
    with jax.named_scope("core"):
        core_copy(every).wait_recv()
    with jax.named_scope("own1"):
        own_score(1)

    def arrive(p, u):
        for by_x in (True, False):
            i = 2 * p + (0 if by_x else 1)

            @if_relay
            def _():
                relay(i)
                if u == 1:
                    k = i - half

                    @pl.when(k < 4 - 2 * x)
                    def _():
                        own_score(2 + k, 0)

                    @pl.when(k < 2)
                    def _():
                        part_score(0, k)

            with jax.named_scope("y"):
                y_copy(i).wait_recv()
            twin_copy(0, u, cut(i)).start()
            with jax.named_scope("x"):
                x_copy(i).wait_recv()
            twin_copy(1, u, cut(i)).start()
            diag_copy(i, by_x).start()

    def two_post(turn, low, size):
        @if_two
        def _():
            @pl.when(two_turn == turn)
            def _():
                two_copy(low, size).start()

    def z_wait(u):
        with jax.named_scope("z"):
            z_copy(u, area(u)).wait_recv()

    for u in range(2):
        each(lambda p: arrive(p, u), u * (half // 2), (u + 1) * (half // 2))
        with jax.named_scope("twin"):
            for k in range(2):
                twin_copy(k, u, area(u)).wait_recv()

        if u == 0:
            two_post(0, 0, unit)

            @unless_relay
            def _():
                with jax.named_scope("own25"):
                    sweep(lambda h: own_score(h, 0), 2, 6 - 2 * x)
                z_wait(0)
                with jax.named_scope("v0"):
                    sweep(lambda h: part_score(0, h), 0, 2)

            @if_relay
            def _():
                z_wait(0)

    def diag_arrive(i):
        diag_copy(i, True).wait_recv()
        twin_copy(2, i // half, cut(i)).start()

    def hand_over():
        @if_relay
        def _():
            with jax.named_scope("relayed"):
                relay_copy(0, every).wait_send()
            pl.semaphore_signal(drained, inc=1, device_id=up, device_id_type=MESH)

        @pl.when(l == 2)
        def _():
            with jax.named_scope("drained"):
                pl.semaphore_wait(drained, 1)
            two_copy(head, unit - head).start()

    def diag_pair(low):
        with jax.named_scope("diag"):
            each(diag_arrive, low, low + 2)

    def steady():
        z_wait(1)
        if wrap:
            two_post(1, 0, head)
        with jax.named_scope("both"):
            sweep(lambda h: both_score(h, 1), 2, 3)
            if wrap:
                hand_over()
            sweep(lambda h: both_score(h, 1), 3, 6 - 2 * x)
            sweep(lambda h: up_score(h, 1), 6 - 2 * x, 6)
        diag_pair(0)
        with jax.named_scope("up"):
            sweep(lambda h: up_score(h, 0), 2, 6)
        diag_pair(2)
        with jax.named_scope("v1"):
            sweep(lambda h: part_score(1, h), 0, 2)

    def delayed():
        with jax.named_scope("own25"):
            sweep(lambda h: own_score(h, 1), 2, 6 - 2 * x)
        with jax.named_scope("v0"):
            sweep(lambda h: part_score(0, h), 2, 6)
        diag_pair(0)
        z_wait(1)

        def later(h):
            @pl.when(h == 2)
            def _():
                diag_pair(2)
            part_score(1, h)

        with jax.named_scope("v1"):
            sweep(later, 0, 6)

    if wrap:
        pl.when(l > 0)(steady)
        pl.when(l == 0)(delayed)
    else:
        steady()
    diag_pair(half)

    def lanes(acc):
        return jnp.max(acc[...].T, axis=0, keepdims=True)

    none = jnp.full((1, rows), -1.0, jnp.float32)

    def back_copy(slot):
        target = cross_up if slot else device(layer(-1), x, r)
        return send(back_out.at[slot], back_in.at[slot], back_send.at[slot], back_recv.at[slot], target)

    def last_score(t):
        u, odd = t // 2, lax.rem(t, 2)

        @pl.when(t == 2)
        def _():
            diag_pair(half + 2)

        @pl.when(odd == 1)
        def _():
            with jax.named_scope("twin2"):
                twin_copy(2, u, area(u)).wait_recv()

        @pl.when(x == 0)
        def _():
            both_score(6 + odd, u)

        @pl.when(x == 1)
        def _():
            up_score(6 + odd, u)

        @if_relay
        def _():
            @pl.when(odd == u)
            def _():
                with jax.named_scope("pair"):
                    pair_score(4 + t - odd)

    with jax.named_scope("last"):
        each(last_score, 0, 4)

    @if_relay
    def _():
        best = lanes(pair_acc)
        back_out[1, 0:1, :] = jnp.where(x == 0, best, none)
        back_out[1, 1:2, :] = jnp.where(x == 0, none, best)
        back_copy(1).start()

    back_out[0, 0:1, :] = none
    back_out[0, 1:2, :] = lanes(guest_acc.at[0])
    back_copy(0).start()

    def twob_copy(k):
        return send(two_out, two_in.at[k], twob_send, twob_recv, device(layer(-2), 1, r))

    def row_copy(h):
        return send(row_out.at[h - 1], row_in.at[h - 1], row_send, row_sem, peer(h))

    def row_post(h):
        row_out[h - 1, 0:1, :] = jnp.max(host_acc[h], axis=0, keepdims=True)
        row_out[h - 1, 1:2, :] = none
        row_copy(h).start()

    @unless_relay
    def _():
        sweep(row_post, 4 - 3 * x, 8 - 4 * x)

    def row_merge(h):
        best = jnp.max(host_acc[h], axis=0, keepdims=True)
        swapped = jnp.max(swap_acc[h - 4], axis=0, keepdims=True)
        row_out[h - 1, 0:1, :] = jnp.where(x == 0, best, jnp.maximum(best, swapped))
        row_out[h - 1, 1:2, :] = jnp.where(x == 0, swapped, none)
        row_copy(h).start()

    @if_relay
    def _():
        sweep(row_merge, 4, 8)
        sweep(row_post, 1, 4)

    @if_two
    def _():
        with jax.named_scope("two"):
            two_copy(0, unit).wait_recv()
        with jax.named_scope("v2"):
            two_score(4 * x)
        two_out[...] = jnp.broadcast_to(lanes(two_acc), two_out.shape)
        twob_copy(x).start()

    with jax.named_scope("rows"):
        @unless_relay
        def _():
            sweep(row_post, 1 + 3 * x, 4 + 4 * x)

    late_ref[...] = jnp.max(host_acc[0], axis=0, keepdims=True)
    early_ref[...] = lanes(guest_acc.at[1])

    def take(best):
        late_ref[...] = jnp.maximum(late_ref[...], best[0:1, :])
        early_ref[...] = jnp.maximum(early_ref[...], best[1:2, :])

    with jax.named_scope("rowin"):
        send(row_out, row_in, row_send, row_sem, peer(1)).wait_recv()
        for h in range(1, 8):
            take(row_in.at[h - 1])
    with jax.named_scope("back"):
        back_copy(0).wait_recv()
        take(back_in.at[0])

        @if_two
        def _():
            @pl.when(x == 1)
            def _():
                send(two_in, two_in, twob_send, twob_recv, far_up).wait_recv()
                for k in range(2):
                    at = slice(k * unit, (k + 1) * unit)
                    early_ref[:, at] = jnp.maximum(early_ref[:, at], two_in[k, 0:1, :])

        if wrap:
            @pl.when(last == 1)
            def _():
                back_copy(1).wait_recv()
                take(back_in.at[1])

    with jax.named_scope("drain"):
        core_copy(every).wait_send()
        x_copy(0, every).wait_send()
        y_copy(0, every).wait_send()
        z_copy(0, every).wait_send()
        diag_copy(0, True, every).wait_send()
        for k in range(3):
            twin_copy(k, 0, every).wait_send()

        @if_two
        def _():
            two_copy(0, unit).wait_send()
            twob_copy(0).wait_send()

        send(row_out, row_in, row_send, row_sem, peer(1)).wait_send()
        back_copy(0).wait_send()

        @if_relay
        def _():
            back_copy(1).wait_send()


def kernel(blocks, copies, *refs):
    dma = pltpu.SemaphoreType.DMA
    pl.run_scoped(
        functools.partial(program, blocks, copies, *refs),
        dma((CHUNKS,)), dma,
        dma, dma, dma, dma((CHUNKS,)), dma, dma((CHUNKS,)), dma, dma((2,)), dma((2 * CHUNKS,)),
        dma, dma, dma((CHUNKS,)), dma((3,)), dma((3, 2)), dma, dma,
        dma, dma, dma((2,)), dma((2,)), dma, dma, pltpu.SemaphoreType.REGULAR,
    )


def shards(embeddings, ranks):
    rows, width = embeddings.shape
    copies = lax.axis_size("rep")
    blocks = lax.axis_size("blk")
    lines = rows // LANES
    vmem = pl.BlockSpec(memory_space=pltpu.VMEM)
    hbm = pl.BlockSpec(memory_space=pltpu.HBM)
    f32, i32, bf16 = jnp.float32, jnp.int32, jnp.bfloat16
    both = pl.pallas_call(
        functools.partial(kernel, blocks, copies),
        out_shape=jax.ShapeDtypeStruct((2, rows), f32),
        in_specs=[hbm, hbm],
        out_specs=vmem,
        scratch_shapes=[
            pltpu.VMEM((rows, width), f32),
            pltpu.VMEM((3, 2 * copies * lines, LANES), i32),
            pltpu.VMEM((9, rows, width), bf16),
            pltpu.VMEM((rows, width), bf16),
            pltpu.VMEM((rows // 2, width), bf16),
            pltpu.VMEM((2, rows, LANES), i32),
            pltpu.VMEM((rows, LANES), i32),
            pltpu.VMEM((rows // 2, LANES), i32),
            pltpu.VMEM((2, rows, LANES), f32),
            pltpu.VMEM((rows, LANES), f32),
            pltpu.VMEM((rows // 2, LANES), f32),
            pltpu.VMEM((8, 8, rows), f32),
            pltpu.VMEM((4, 8, rows), f32),
            pltpu.VMEM((7, 2, rows), f32),
            pltpu.VMEM((7, 2, rows), f32),
            pltpu.VMEM((2, 2, rows), f32),
            pltpu.VMEM((2, 2, rows), f32),
            pltpu.VMEM((2, rows // 2), f32),
            pltpu.VMEM((2, 2, rows // 2), f32),
        ],
        compiler_params=pltpu.CompilerParams(
            collective_id=0, has_side_effects=True, vmem_limit_bytes=56_500_000
        ),
    )(embeddings, ranks.reshape(-1, LANES))
    return both[0], both[1]


def solution(mesh):
    return jax.shard_map(
        shards,
        mesh=mesh,
        in_specs=(P(("blk", "rep"), None), P()),
        out_specs=(P(("blk", "rep")), P(("blk", "rep"))),
        check_vma=False,
    )
```
